128 devices in a mesh: row: 16 (over z_lo, x, core), col: 4 (over y), head: 2 (over z_hi).
Axes of the slice: x: 4, y: 4, z: 4 (z_hi: 2, z_lo: 2; z = z_hi * 2 + z_lo), core: 2. Of those that a mesh axis runs over, the one named last changes fastest.
Arguments:
- query_map: bfloat16 [256, 128, 3072], P('row', 'col', 'head'), may hold values from -6 to 6
- key_map: bfloat16 [256, 128, 3072], P('row', 'col', 'head'), may hold values from -7 to 7
- value_map: bfloat16 [256, 128, 3072], P('row', 'col', 'head'), may hold values from -6 to 6
- window_mask: int32 [16, 4, 13, 13], P('row', 'col'), may hold values 0 or 1
- tile_radius: int32 [16, 4], P('row', 'col'), may hold values from 3 to 6, as said below
- dilation_per_tile: int32 [16, 4], P('row', 'col'), may hold values from 1 to 3, as said below
- rel_bias: float32 [48, 13, 13], P('head'), may hold values from -4 to 4
- out_weight: bfloat16 [3072, 3072], P('head'), may hold values from -0.109375 to 0.109375
Outputs:
- mixed: bfloat16 [256, 128, 3072], P('row', 'col', 'head')
The draws below stay inside these ranges and needn't reach their ends.
Inputs may be any that keep to these rules, and one draw needn't show every extreme that they name: `tile_radius`: in each row of tiles, at least one tile has radius 6 and dilation 3. `dilation_per_tile`: in each row of tiles, at least one tile has radius 6 and dilation 3.
All inputs are finite; a program needn't handle non-finite values. No bound on the sum of `window_mask` on one device may be relied on, other than what follows from the above.
Results may differ from the reference program's by a relative error of at most 0.0073.
Values may be sent and summed in bfloat16 or wider, within the bound.
A program may use at most 384 MiB of HBM per device.

```python
import math
from functools import partial
import jax
import jax.numpy as jnp
from jax import lax

TILE_ROWS = 16
TILE_COLS = 32
HEADS = 48
HEAD_DIM = 64
RADIUS_MAX = 6
DILATION_LIMIT = 3
WINDOW = 13
HALO = 18
FEATURES = 3072
MODEL = 3072
ROWS = 256
COLS = 128
N_ROW = 16
N_COL = 4


def draw_query_map(key, part):
    drawn = jax.random.normal(jax.random.fold_in(key, 3), (ROWS, COLS, FEATURES), jnp.float32)
    return jnp.clip(drawn, -6.0, 6.0).astype(jnp.bfloat16)


def draw_key_map(key, part):
    drawn = jax.random.normal(jax.random.fold_in(key, 5), (ROWS, COLS, FEATURES), jnp.float32)
    return jnp.clip(drawn, -6.0, 6.0).astype(jnp.bfloat16)


def window_settings(key):
    base = jax.random.fold_in(key, 29)
    pick_key, radius_key, dilation_key = jax.random.split(base, 3)
    chosen_col = jax.random.randint(pick_key, (N_ROW,), 0, N_COL)
    radius = jax.random.randint(radius_key, (N_ROW, N_COL), 3, RADIUS_MAX + 1)
    dilation = jax.random.randint(dilation_key, (N_ROW, N_COL), 1, DILATION_LIMIT + 1)
    widest = jnp.arange(N_COL, dtype=jnp.int32)[None, :] == chosen_col[:, None]
    radius = jnp.where(widest, RADIUS_MAX, radius).astype(jnp.int32)
    dilation = jnp.where(widest, DILATION_LIMIT, dilation).astype(jnp.int32)
    return (radius, dilation)


def draw_tile_radius(key, part):
    return window_settings(key)[0]


def draw_dilation_per_tile(key, part):
    return window_settings(key)[1]


def touch_ends(result, own_key, smallest, top_value):
    index_at = [jax.random.randint(jax.random.fold_in(own_key, axis), (), 0, length) for axis, length in enumerate(result.shape)]
    longest = result.shape.index(max(result.shape))
    next_to = index_at[:longest] + [(index_at[longest] + 1) % result.shape[longest]] + index_at[longest + 1:]
    return result.at[tuple(index_at)].set(smallest).at[tuple(next_to)].set(top_value)


def shard_levels(key, shape, cuts, low, high):
    gain, own = 1.0, jax.random.fold_in(key, 6)
    for position, parts in cuts:
        draws = jnp.exp(jax.random.uniform(jax.random.fold_in(own, position), (parts,), jnp.float32, low / len(cuts), high / len(cuts)))
        gain = gain * jnp.repeat(draws, shape[position] // parts).reshape([-1 if axis == position else 1 for axis in range(len(shape))])
    return gain


def gaussian(rng, dims, width, limit, pieces=(), kind=jnp.bfloat16):
    values = width * jax.random.normal(rng, dims, jnp.float32)
    if pieces:
        values = values * shard_levels(rng, dims, pieces, -0.22, 0.18)
    return jnp.clip(values, -limit, limit).astype(kind)


def setup_inputs(seed: int = 0) -> dict:
    keys = jax.random.split(jax.random.key(seed), 9)
    query_map = draw_query_map(jax.random.fold_in(keys[8], 71), 0)
    key_map = draw_key_map(jax.random.fold_in(keys[8], 71), 0)
    value_map = gaussian(keys[2], (ROWS, COLS, FEATURES), 1.0, 6.0, ((0, 16), (1, 4), (2, 2)))
    window_mask = touch_ends((jax.random.randint(keys[3], (N_ROW, N_COL, WINDOW, WINDOW), 0, 4) < 3).astype(jnp.int32), jax.random.fold_in(keys[3], 1), 0, 1)
    tile_radius = draw_tile_radius(jax.random.fold_in(keys[8], 71), 0)
    dilation_per_tile = draw_dilation_per_tile(jax.random.fold_in(keys[8], 71), 0)
    rel_bias = gaussian(keys[6], (HEADS, WINDOW, WINDOW), 1.0, 4.0, ((0, 2),), jnp.float32)
    out_weight = gaussian(keys[7], (FEATURES, MODEL), FEATURES ** -0.5, 0.109375, ((0, 2),))
    return {"query_map": query_map, "key_map": key_map, "value_map": value_map, "window_mask": window_mask, "tile_radius": tile_radius, "dilation_per_tile": dilation_per_tile, "rel_bias": rel_bias, "out_weight": out_weight}


def tile_attention(index, query_map, padded_keys, padded_values, window_mask, tile_radius, dilation_per_tile, rel_bias):
    tile_row = index // N_COL
    tile_col = index % N_COL
    row_anchor = tile_row * TILE_ROWS
    col_anchor = tile_col * TILE_COLS
    zero_index = jnp.int32(0)
    queries = lax.dynamic_slice(query_map, (row_anchor, col_anchor, zero_index), (TILE_ROWS, TILE_COLS, FEATURES))
    queries = queries.astype(jnp.float32).reshape(TILE_ROWS, TILE_COLS, HEADS, HEAD_DIM)
    key_block = lax.dynamic_slice(padded_keys, (row_anchor, col_anchor, zero_index), (TILE_ROWS + 2 * HALO, TILE_COLS + 2 * HALO, FEATURES))
    value_block = lax.dynamic_slice(padded_values, (row_anchor, col_anchor, zero_index), (TILE_ROWS + 2 * HALO, TILE_COLS + 2 * HALO, FEATURES))
    radius = tile_radius[tile_row, tile_col]
    dilation = dilation_per_tile[tile_row, tile_col]
    pattern = window_mask[tile_row, tile_col]
    rows_here = row_anchor + jnp.arange(TILE_ROWS, dtype=jnp.int32)
    cols_here = col_anchor + jnp.arange(TILE_COLS, dtype=jnp.int32)
    score_scale = 1.0 / math.sqrt(HEAD_DIM)
    score_list = []
    mask_list = []
    starts = []
    for row_step in range(-RADIUS_MAX, RADIUS_MAX + 1):
        for col_step in range(-RADIUS_MAX, RADIUS_MAX + 1):
            row_start = HALO + row_step * dilation
            col_start = HALO + col_step * dilation
            starts.append((row_start, col_start))
            shifted = lax.dynamic_slice(key_block, (row_start, col_start, zero_index), (TILE_ROWS, TILE_COLS, FEATURES))
            shifted = shifted.astype(jnp.float32).reshape(TILE_ROWS, TILE_COLS, HEADS, HEAD_DIM)
            score = lax.optimization_barrier(jnp.sum(queries * shifted, axis=-1)) * score_scale
            score = score + rel_bias[:, row_step + RADIUS_MAX, col_step + RADIUS_MAX][None, None, :]
            inside = pattern[row_step + RADIUS_MAX, col_step + RADIUS_MAX] == 1
            if row_step == 0 and col_step == 0:
                inside = jnp.logical_or(inside, True)
            inside = inside & (abs(row_step) <= radius) & (abs(col_step) <= radius)
            row_global = rows_here + row_step * dilation
            col_global = cols_here + col_step * dilation
            row_fine = (row_global >= 0) & (row_global < ROWS)
            column_offset = (col_global >= 0) & (col_global < COLS)
            mask_list.append(inside & row_fine[:, None] & column_offset[None, :])
            score_list.append(score)
    scores = jnp.stack(score_list)
    masks = jnp.stack(mask_list)[..., None]
    peak_score = lax.optimization_barrier(jnp.max(jnp.where(masks, scores, -1e+30), axis=0, keepdims=True))
    exponent = jnp.where(masks, jnp.exp(jnp.where(masks, scores - peak_score, -60.0)), 0.0)
    denominator = lax.optimization_barrier(jnp.sum(exponent, axis=0, keepdims=True))
    weights = (exponent / denominator).astype(jnp.bfloat16)
    attended = jnp.zeros((TILE_ROWS, TILE_COLS, HEADS, HEAD_DIM), jnp.float32)
    for place in range(len(starts)):
        row_start, col_start = starts[place]
        shifted = lax.dynamic_slice(value_block, (row_start, col_start, zero_index), (TILE_ROWS, TILE_COLS, FEATURES))
        shifted = shifted.astype(jnp.float32).reshape(TILE_ROWS, TILE_COLS, HEADS, HEAD_DIM)
        attended = attended + weights[place].astype(jnp.float32)[..., None] * shifted
    return attended.reshape(TILE_ROWS, TILE_COLS, FEATURES).astype(jnp.bfloat16)

def reference(query_map, key_map, value_map, window_mask, tile_radius, dilation_per_tile, rel_bias, out_weight):
    padding = ((HALO, HALO), (HALO, HALO), (0, 0))
    padded_keys = jnp.pad(key_map, padding)
    padded_values = jnp.pad(value_map, padding)
    worker = partial(tile_attention, query_map=query_map, padded_keys=padded_keys, padded_values=padded_values, window_mask=window_mask, tile_radius=tile_radius, dilation_per_tile=dilation_per_tile, rel_bias=rel_bias)
    tiles = lax.map(worker, jnp.arange(N_ROW * N_COL, dtype=jnp.int32))
    tiles = tiles.reshape(N_ROW, N_COL, TILE_ROWS, TILE_COLS, FEATURES).transpose(0, 2, 1, 3, 4)
    attended = tiles.reshape(ROWS * COLS, FEATURES)
    mixed = jnp.dot(attended, out_weight, preferred_element_type=jnp.float32).astype(jnp.bfloat16)
    return mixed.reshape(ROWS, COLS, MODEL)
```

```python
import functools

import jax
import jax.numpy as jnp
from jax import lax
from jax.experimental import pallas as pl
from jax.experimental.pallas import tpu as pltpu
from jax.sharding import PartitionSpec as P

HEAD_DIM = 64
RADIUS_MAX = 6
WINDOW = 13
HALO = 18
NEG = -1e30
BLOCK_ROWS = 3
BLOCK_KEYS = 16
SIDE_COLS = 24
GROUP = 4
LANES = GROUP * HEAD_DIM
CHUNKS = 3


def shifted(value, axis, steps):
    count = lax.axis_size(axis)
    leading, last = (max(0, -steps), min(count, count - steps))
    return lax.ppermute(value, axis, [(source, source + steps) for source in range(leading, last)])


def table_kernel(cols, offset, d_ref, x_ref, t_ref):
    d = d_ref[0]
    width = x_ref.shape[2]
    lane = lax.broadcasted_iota(jnp.int32, (cols, width), 1)
    rel = lane % 32 - lax.broadcasted_iota(jnp.int32, (cols, width), 0) + offset

    @pl.loop(0, x_ref.shape[0])
    def _(h):
        rows = x_ref[h]
        for t in range(BLOCK_ROWS):
            acc = jnp.full((cols, width), NEG, jnp.float32)
            for b in range(WINDOW):
                row = rows[t * WINDOW + b : t * WINDOW + b + 1]
                acc = jnp.where(rel == (b - RADIUS_MAX) * d, row, acc)
            t_ref[h, t] = acc


def make_table(cols, offset, pattern, radius, dilation, rel_bias):
    heads = rel_bias.shape[0]
    steps = jnp.abs(jnp.arange(WINDOW, dtype=jnp.int32) - RADIUS_MAX)
    centre = (steps[:, None] == 0) & (steps[None, :] == 0)
    near = (steps[:, None] <= radius) & (steps[None, :] <= radius)
    used = ((pattern == 1) | centre) & near
    masked = jnp.where(used[None], rel_bias, NEG)
    turned = jnp.swapaxes(masked, 1, 2)
    extra = BLOCK_KEYS - WINDOW
    turned = jnp.pad(turned, ((0, 0), (0, 0), (BLOCK_ROWS - 1, extra)), constant_values=NEG)
    parts = [turned[:, :, BLOCK_ROWS - 1 - t :][:, :, :BLOCK_KEYS] for t in range(BLOCK_ROWS)]
    flat = jnp.stack(parts, axis=1).reshape(heads * BLOCK_ROWS * WINDOW, BLOCK_KEYS)
    width = BLOCK_KEYS * 32
    lane_row = jnp.arange(width, dtype=jnp.int32)[None, :] // 32
    spread = (lane_row == jnp.arange(BLOCK_KEYS, dtype=jnp.int32)[:, None]).astype(jnp.float32)
    wide = jnp.dot(flat, spread, precision=lax.Precision.HIGHEST)
    wide = wide.reshape(heads, BLOCK_ROWS * WINDOW, width)
    return pl.pallas_call(
        functools.partial(table_kernel, cols, offset),
        grid=(heads // GROUP,),
        in_specs=[
            pl.BlockSpec(memory_space=pltpu.SMEM),
            pl.BlockSpec((GROUP, BLOCK_ROWS * WINDOW, width), lambda g: (g, 0, 0)),
        ],
        out_specs=pl.BlockSpec((GROUP, BLOCK_ROWS, cols, width), lambda g: (g, 0, 0, 0)),
        out_shape=jax.ShapeDtypeStruct((heads, BLOCK_ROWS, cols, width), jnp.float32),
        cost_estimate=pl.CostEstimate(flops=10**9, bytes_accessed=10**7, transcendentals=0),
        name="bias_table",
    )(dilation.reshape(1), wide)


def one_set(cols, d, row_anchor, total_rows, head0, beta, q_ref, t_ref, o_ref, l_ref, k_ref, v_ref, s_ref, p_ref):
    base = beta % d + BLOCK_ROWS * d * (beta // d)
    depth = o_ref.shape[0]
    span = k_ref.shape[0]
    width = BLOCK_KEYS * 32
    queries = []
    for t in range(BLOCK_ROWS):
        row = jnp.minimum(base + t * d, depth - 1)
        queries.append(q_ref[row].astype(jnp.float32) * 0.125)
    queries = jnp.concatenate(queries, axis=0)
    lane_head = lax.broadcasted_iota(jnp.int32, queries.shape, 1) // HEAD_DIM
    spread = [jnp.where(lane_head == h, queries, 0.0) for h in range(GROUP)]
    spread = jnp.concatenate(spread, axis=0).astype(jnp.bfloat16)
    key_rows = []
    value_rows = []
    for u in range(BLOCK_KEYS):
        row = jnp.clip(HALO + base + (u - RADIUS_MAX) * d, 0, span - 1)
        key_rows.append(k_ref[row])
        value_rows.append(v_ref[row])
    keys = jnp.concatenate(key_rows, axis=0)
    values = jnp.concatenate(value_rows, axis=0)
    s_ref[...] = lax.dot_general(
        spread, keys, (((1,), (1,)), ((), ())), preferred_element_type=jnp.float32
    )
    step = lax.broadcasted_iota(jnp.int32, (1, width), 1) // 32
    key_row = row_anchor + base + (step - RADIUS_MAX) * d
    row_bias = jnp.where((key_row >= 0) & (key_row < total_rows), 0.0, NEG)
    sums = []
    peaks = []
    for h in range(GROUP):
        for t in range(BLOCK_ROWS):
            at = (h * BLOCK_ROWS + t) * cols
            score = s_ref[at : at + cols] + (t_ref[h, t] + row_bias)
            peak = jnp.maximum(jnp.max(score, axis=1, keepdims=True), -1e20)
            weight = jnp.exp(score - peak)
            sums.append(jnp.sum(weight, axis=1, keepdims=True))
            peaks.append(peak)
            p_ref[at : at + cols] = weight.astype(jnp.bfloat16)
    mixed = jnp.dot(p_ref[...], values, preferred_element_type=jnp.float32)
    head_of = lax.broadcasted_iota(jnp.int32, (cols, LANES), 1) // HEAD_DIM
    stat_lane = lax.broadcasted_iota(jnp.int32, (cols, 128), 1)
    for t in range(BLOCK_ROWS):
        row = base + t * d
        out = jnp.zeros((cols, LANES), jnp.float32)
        stats = l_ref[jnp.minimum(row, depth - 1)]
        for h in range(GROUP):
            at = h * BLOCK_ROWS + t
            total = sums[at]
            some = total > 0.0
            inverse = 1.0 / jnp.where(some, total, 1.0)
            out = jnp.where(head_of == h, mixed[at * cols : (at + 1) * cols] * inverse, out)
            lse = jnp.where(some, peaks[at] + jnp.log(jnp.where(some, total, 1.0)), NEG)
            stats = jnp.where(stat_lane == head0 + h, lse, stats)

        @pl.when(row < depth)
        def _():
            o_ref[row] = out.astype(o_ref.dtype)
            l_ref[row] = stats


def attention_kernel(
    chunk_head0, total_rows, tiny,
    q_o, q_l, q_r, own_k, own_v, up_far, up, down, down_far, t_o, t_l, t_r,
    o_o, o_l, o_r, l_o, l_l, l_r, k_ref, v_ref, s_o, s_l, s_r, p_o, p_l, p_r,
):
    group = pl.program_id(0)
    depth = own_k.shape[0]
    spill = HALO - depth
    for which, (ref, own) in enumerate(((k_ref, own_k), (v_ref, own_v))):
        ref[0:spill] = up_far[which]
        ref[spill:HALO] = up[which]
        ref[HALO : HALO + depth] = own[...]
        ref[HALO + depth : HALO + 2 * depth] = down[which]
        ref[HALO + 2 * depth : 2 * HALO + depth] = down_far[which]

    @pl.when(group == 0)
    def _():
        for ref in (l_o, l_l, l_r):
            ref[...] = jnp.zeros_like(ref)

    head0 = chunk_head0 + group * GROUP
    sets = (
        (tiny[0], q_o, t_o, o_o, l_o, s_o, p_o),
        (tiny[1], q_l, t_l, o_l, l_l, s_l, p_l),
        (tiny[2], q_r, t_r, o_r, l_r, s_r, p_r),
    )

    @pl.loop(0, 6)
    def _(beta):
        for d, q, t, o, l, s, p in sets:
            one_set(q.shape[1], d, tiny[3], total_rows, head0, beta, q, t, o, l, k_ref, v_ref, s, p)


def attention(chunk, tiny, total_rows, q, q_l, q_r, k, v, halo, tables):
    depth, cols, _ = q.shape
    width = q_l.shape[2]
    groups = width // LANES
    first = chunk * groups
    side = q_l.shape[1]
    up_far, up, down, down_far = halo
    whole = lambda arr: pl.BlockSpec(arr.shape[:-1] + (LANES,), lambda g: (0,) * (arr.ndim - 1) + (g,))
    offset = lambda arr: pl.BlockSpec(arr.shape[:-1] + (LANES,), lambda g: (0, 0, g + first))
    table = lambda arr: pl.BlockSpec((GROUP,) + arr.shape[1:], lambda g: (g + first, 0, 0, 0))
    stats = lambda n: pl.BlockSpec((depth, n, 128), lambda g: (0, 0, 0))
    outs = lambda n: pl.BlockSpec((depth, n, LANES), lambda g: (0, 0, g))
    rows = lambda n: GROUP * BLOCK_ROWS * n
    keys = BLOCK_KEYS * 32
    return pl.pallas_call(
        functools.partial(attention_kernel, chunk * groups * GROUP, total_rows),
        grid=(groups,),
        in_specs=[pl.BlockSpec(memory_space=pltpu.SMEM), offset(q), whole(q_l), whole(q_r)]
        + [offset(k), offset(v)]
        + [whole(part) for part in halo]
        + [table(part) for part in tables],
        out_specs=[outs(cols), outs(side), outs(side), stats(cols), stats(side), stats(side)],
        out_shape=[jax.ShapeDtypeStruct((depth, n, width), jnp.bfloat16) for n in (cols, side, side)]
        + [jax.ShapeDtypeStruct((depth, n, 128), jnp.float32) for n in (cols, side, side)],
        scratch_shapes=[pltpu.VMEM((depth + 2 * HALO, cols, LANES), jnp.bfloat16)] * 2
        + [pltpu.VMEM((rows(n), keys), jnp.float32) for n in (cols, side, side)]
        + [pltpu.VMEM((rows(n), keys), jnp.bfloat16) for n in (cols, side, side)],
        compiler_params=pltpu.CompilerParams(vmem_limit_bytes=56 * 2**20),
        cost_estimate=pl.CostEstimate(flops=6 * 10**9, bytes_accessed=2 * 10**7, transcendentals=0),
        name="window_attention",
    )(tiny, q, q_l, q_r, k, v, up_far, up, down, down_far, *tables)


def merge_kernel(places, has_left, has_right, *refs):
    own, left, right = refs[:CHUNKS], refs[CHUNKS : 2 * CHUNKS], refs[2 * CHUNKS : 3 * CHUNKS]
    l_o, l_l, l_r, w_ref, a_ref, part_ref = refs[3 * CHUNKS :]
    rows, cols, width = own[0].shape
    features = width * CHUNKS
    pick = lax.broadcasted_iota(jnp.int32, (128, features), 1) // HEAD_DIM
    pick = (pick == lax.broadcasted_iota(jnp.int32, (128, features), 0)).astype(jnp.bfloat16)
    tail = cols - l_l.shape[1]

    def lay(ref, i, ahead, fill):
        value = ref[i].astype(jnp.float32)
        blank = jnp.full((tail, value.shape[1]), fill, jnp.float32)
        return jnp.concatenate([blank, value] if ahead else [value, blank], axis=0)

    first, second, third = [], [], []
    for i in range(rows):
        a = l_o[i]
        b = jnp.where(has_left[0] > 0, lay(l_l, i, False, NEG), NEG)
        c = jnp.where(has_right[0] > 0, lay(l_r, i, True, NEG), NEG)
        top = jnp.maximum(jnp.maximum(a, b), c)
        a, b, c = jnp.exp(a - top), jnp.exp(b - top), jnp.exp(c - top)
        total = a + b + c
        first.append(a / total)
        second.append(b / total)
        third.append(c / total)

    def wide(parts):
        value = jnp.concatenate(parts, axis=0)
        high = value.astype(jnp.bfloat16)
        low = (value - high.astype(jnp.float32)).astype(jnp.bfloat16)
        dot = lambda x: jnp.dot(x, pick, preferred_element_type=jnp.float32)
        return dot(high) + dot(low)

    def gather(chunks, ahead):
        found = []
        for i in range(rows):
            if ahead is None:
                found.append(jnp.concatenate([ref[i].astype(jnp.float32) for ref in chunks], axis=1))
            else:
                found.append(jnp.concatenate([lay(ref, i, ahead, 0.0) for ref in chunks], axis=1))
        return jnp.concatenate(found, axis=0)

    total = wide(first) * gather(own, None)
    total = total + wide(second) * gather(left, False)
    total = total + wide(third) * gather(right, True)
    attended = total.astype(jnp.bfloat16)
    a_ref[...] = attended
    part_ref[...] = jnp.dot(attended, w_ref[...], preferred_element_type=jnp.float32).astype(jnp.bfloat16)


def merge(peer, has_left, has_right, own, left, right, stats, weight):
    depth, cols, width = own[0].shape
    rows = 4
    half = weight.shape[1] // 2
    features = weight.shape[0]
    by_row = lambda arr: pl.BlockSpec((rows,) + arr.shape[1:], lambda i, *_: (i, 0, 0))
    flat = lambda n: pl.BlockSpec((rows * cols, n), lambda i, *_: (i, 0))
    return pl.pallas_call(
        merge_kernel,
        grid_spec=pltpu.PrefetchScalarGridSpec(
            num_scalar_prefetch=3,
            grid=(depth // rows,),
            in_specs=[by_row(arr) for arr in (*own, *left, *right, *stats)]
            + [pl.BlockSpec((features, half), lambda i, p, *_: (0, p[0]))],
            out_specs=[flat(features), flat(half)],
        ),
        out_shape=[
            jax.ShapeDtypeStruct((depth * cols, features), jnp.bfloat16),
            jax.ShapeDtypeStruct((depth * cols, half), jnp.bfloat16),
        ],
        compiler_params=pltpu.CompilerParams(vmem_limit_bytes=56 * 2**20),
        cost_estimate=pl.CostEstimate(flops=3 * 10**9, bytes_accessed=2 * 10**7, transcendentals=0),
        name="merge_project",
    )(peer, has_left, has_right, *own, *left, *right, *stats, weight)


def shards(query_map, key_map, value_map, window_mask, tile_radius, dilation_per_tile, rel_bias, out_weight):
    depth, cols, features = query_map.shape
    row_anchor = lax.axis_index("row") * depth
    total_rows = depth * lax.axis_size("row")
    spill = HALO - depth
    width = features // CHUNKS
    settings = jnp.concatenate(
        [window_mask.reshape(-1), tile_radius.reshape(-1), dilation_per_tile.reshape(-1)]
    )
    halos = []
    sides = []
    from_left = shifted(settings, "col", 1)
    from_right = shifted(settings, "col", -1)
    for chunk in range(CHUNKS):
        at = slice(chunk * width, (chunk + 1) * width)
        pair = jnp.stack([key_map[:, :, at], value_map[:, :, at]])
        q_l = shifted(query_map[:, cols - SIDE_COLS :, at], "col", 1)
        q_r = shifted(query_map[:, :SIDE_COLS, at], "col", -1)
        up = shifted(pair, "row", 1)
        down = shifted(pair, "row", -1)
        up_far = shifted(pair[:, depth - spill :], "row", 2)
        down_far = shifted(pair[:, :spill], "row", -2)
        halos.append((up_far, up, down, down_far))
        sides.append((q_l, q_r))
    tables = []
    dilations = []
    for values, count, offset in (
        (settings, cols, 0),
        (from_left, SIDE_COLS, SIDE_COLS),
        (from_right, SIDE_COLS, -cols),
    ):
        pattern = values[:-2].reshape(WINDOW, WINDOW)
        dilation = jnp.maximum(values[-1], 1)
        tables.append(make_table(count, offset, pattern, values[-2], dilation, rel_bias))
        dilations.append(dilation)
    tiny = jnp.stack(dilations + [row_anchor]).astype(jnp.int32)
    own, left, right, stats = [], [], [], []
    for chunk in range(CHUNKS):
        o_o, o_l, o_r, *lse = attention(
            chunk, tiny, total_rows, query_map, *sides[chunk], key_map, value_map, halos[chunk], tables
        )
        own.append(o_o)
        left.append(shifted(o_r, "col", 1))
        right.append(shifted(o_l, "col", -1))
        stats.append(lse)
    l_o, l_l, l_r = [sum(parts) for parts in zip(*stats)]
    l_from_left = shifted(l_r, "col", 1)
    l_from_right = shifted(l_l, "col", -1)
    col = lax.axis_index("col")
    head = lax.axis_index("head")
    one = lambda flag: flag.astype(jnp.int32).reshape(1)
    attended, theirs = merge(
        one(1 - head), one(col > 0), one(col < lax.axis_size("col") - 1),
        own, left, right, (l_o, l_from_left, l_from_right), out_weight,
    )
    arrived = lax.ppermute(theirs, "head", [(0, 1), (1, 0)])
    half = out_weight.shape[1] // 2
    my_weight = lax.dynamic_slice_in_dim(out_weight, head * half, half, 1)
    mine = jnp.dot(attended, my_weight, preferred_element_type=jnp.float32)
    mine, arrived = lax.optimization_barrier((mine, arrived))
    return (mine + arrived.astype(jnp.float32)).astype(jnp.bfloat16).reshape(depth, cols, half)


def solution(mesh):
    placed = (
        P("row", "col", "head"),
        P("row", "col", "head"),
        P("row", "col", "head"),
        P("row", "col", None, None),
        P("row", "col"),
        P("row", "col"),
        P("head", None, None),
        P("head", None),
    )
    return jax.shard_map(
        shards, mesh=mesh, in_specs=placed, out_specs=P("row", "col", "head"), check_vma=False
    )
```

```python
import functools

import jax
import jax.numpy as jnp
from jax import lax
from jax.experimental import pallas as pl
from jax.experimental.pallas import tpu as pltpu
from jax.sharding import PartitionSpec as P

HEAD_DIM = 64
RADIUS_MAX = 6
WINDOW = 13
HALO = 18
NEG = -1e30
BLOCK_ROWS = 3
BLOCK_KEYS = 16
SIDE_COLS = 24
GROUP = 4
LANES = GROUP * HEAD_DIM
BLOCKS = 6
SLOTS = BLOCKS * BLOCK_ROWS


MESH = pl.DeviceIdType.MESH


def shifted(value, axis, steps):
    count = lax.axis_size(axis)
    leading, last = (max(0, -steps), min(count, count - steps))
    return lax.ppermute(value, axis, [(source, source + steps) for source in range(leading, last)])


def spread_bias(pattern, radius, rel_bias, first, last):
    heads = rel_bias.shape[0]
    steps = jnp.abs(jnp.arange(WINDOW, dtype=jnp.int32) - RADIUS_MAX)
    centre = (steps[:, None] == 0) & (steps[None, :] == 0)
    near = (steps[:, None] <= radius) & (steps[None, :] <= radius)
    used = ((pattern == 1) | centre) & near
    masked = jnp.where(used[None], rel_bias, NEG)
    turned = jnp.swapaxes(masked, 1, 2)[:, first:last]
    extra = BLOCK_KEYS - WINDOW
    turned = jnp.pad(turned, ((0, 0), (0, 0), (BLOCK_ROWS - 1, extra)), constant_values=NEG)
    parts = [turned[:, :, BLOCK_ROWS - 1 - t :][:, :, :BLOCK_KEYS] for t in range(BLOCK_ROWS)]
    count = BLOCK_ROWS * (last - first)
    flat = jnp.stack(parts, axis=1).reshape(heads * count, BLOCK_KEYS)
    width = BLOCK_KEYS * 32
    lane_row = jnp.arange(width, dtype=jnp.int32)[None, :] // 32
    spread = (lane_row == jnp.arange(BLOCK_KEYS, dtype=jnp.int32)[:, None]).astype(jnp.float32)
    wide = jnp.dot(flat, spread, precision=lax.Precision.HIGHEST)
    return wide.reshape(heads, count, width)


def fill_table(cols, offset, first, last, d, x_ref, t_ref):
    width = x_ref.shape[2]
    lane = lax.broadcasted_iota(jnp.int32, (cols, width), 1)
    rel = lane % 32 - lax.broadcasted_iota(jnp.int32, (cols, width), 0) + offset
    count = last - first

    @pl.loop(0, x_ref.shape[0])
    def _(h):
        rows = x_ref[h]
        for t in range(BLOCK_ROWS):
            acc = jnp.full((cols, width), NEG, jnp.float32)
            for b in range(count):
                row = rows[t * count + b : t * count + b + 1]
                acc = jnp.where(rel == (b + first - RADIUS_MAX) * d, row, acc)
            t_ref[h, t] = acc


def base_row(beta, d):
    two = beta % 2 + 6 * (beta // 2)
    three = beta % 3 + 9 * (beta // 3)
    return jnp.where(d == 1, 3 * beta, jnp.where(d == 2, two, three))


def one_set(d, row_anchor, total_rows, group, beta, load_q, t_ref, store_o, l_ref, k_ref, v_ref, s_ref, p_ref):
    cols = t_ref.shape[2]
    base = base_row(beta, d)
    span = k_ref.shape[0]
    depth = span - 2 * HALO
    width = BLOCK_KEYS * 32
    queries = []
    for t in range(BLOCK_ROWS):
        row = jnp.minimum(base + t * d, depth - 1)
        queries.append(load_q(row).astype(jnp.float32) * 0.125)
    queries = jnp.concatenate(queries, axis=0)
    lane_head = lax.broadcasted_iota(jnp.int32, queries.shape, 1) // HEAD_DIM
    spread = [jnp.where(lane_head == h, queries, 0.0) for h in range(GROUP)]
    spread = jnp.concatenate(spread, axis=0).astype(jnp.bfloat16)
    key_rows = []
    value_rows = []
    for u in range(BLOCK_KEYS):
        row = jnp.clip(HALO + base + (u - RADIUS_MAX) * d, 0, span - 1)
        key_rows.append(k_ref[row])
        value_rows.append(v_ref[row])
    keys = jnp.concatenate(key_rows, axis=0)
    values = jnp.concatenate(value_rows, axis=0)
    s_ref[...] = lax.dot_general(
        spread, keys, (((1,), (1,)), ((), ())), preferred_element_type=jnp.float32
    )
    step = lax.broadcasted_iota(jnp.int32, (1, width), 1) // 32
    key_row = row_anchor + base + (step - RADIUS_MAX) * d
    row_bias = jnp.where((key_row >= 0) & (key_row < total_rows), 0.0, NEG)
    sums = []
    peaks = []
    for h in range(GROUP):
        for t in range(BLOCK_ROWS):
            at = (h * BLOCK_ROWS + t) * cols
            score = s_ref[at : at + cols] + (t_ref[group * GROUP + h, t] + row_bias)
            peak = jnp.maximum(jnp.max(score, axis=1, keepdims=True), -1e20)
            weight = jnp.exp(score - peak)
            sums.append(jnp.sum(weight, axis=1, keepdims=True))
            peaks.append(peak)
            p_ref[at : at + cols] = weight.astype(jnp.bfloat16)
    mixed = jnp.dot(p_ref[...], values, preferred_element_type=jnp.float32)
    head_of = lax.broadcasted_iota(jnp.int32, (cols, LANES), 1) // HEAD_DIM
    stat_lane = lax.broadcasted_iota(jnp.int32, (cols, 128), 1)
    for t in range(BLOCK_ROWS):
        slot = beta * BLOCK_ROWS + t
        out = jnp.zeros((cols, LANES), jnp.float32)
        stats = l_ref[slot]
        for h in range(GROUP):
            at = h * BLOCK_ROWS + t
            total = sums[at]
            some = total > 0.0
            inverse = 1.0 / jnp.where(some, total, 1.0)
            out = jnp.where(head_of == h, mixed[at * cols : (at + 1) * cols] * inverse, out)
            lse = jnp.where(some, peaks[at] + jnp.log(jnp.where(some, total, 1.0)), NEG)
            stats = jnp.where(stat_lane == group * GROUP + h, lse, stats)
        store_o(slot, out.astype(jnp.bfloat16))
        l_ref[slot] = stats


def window_kernel(
    total_rows, groups, tiny, q_ref, k_own, v_own, x_o, x_l, x_r,
    o_own, l_own, back_l, back_r, lse_l, lse_r,
    win_k, win_v, k_ref, v_ref, land_l, land_r, q_l, q_r, t_o, t_l, t_r,
    s_o, s_l, s_r, p_o, p_l, p_r, out_l, out_r, st_l, st_r,
    send, recv, back_send, back_recv,
):
    row, col = lax.axis_index("row"), lax.axis_index("col")
    rows, cols_n = lax.axis_size("row"), lax.axis_size("col")
    depth, cols, _ = k_own.shape
    spill = HALO - depth
    side = land_l.shape[2]

    for edge, at, n in (
        (row < 2, 0, spill),
        (row < 1, spill, depth),
        (row > rows - 2, HALO, depth),
        (row > rows - 3, HALO + depth, spill),
    ):
        @pl.when(edge)
        def _():
            for ref in (win_k, win_v):
                ref[:, at : at + n] = jnp.zeros((groups, n, cols, LANES), ref.dtype)
    for edge, ref in ((col < 1, land_l), (col > cols_n - 2, land_r)):
        @pl.when(edge)
        def _():
            ref[...] = jnp.zeros_like(ref)

    peers = (
        (row < rows - 1, {"row": row + 1}),
        (row > 0, {"row": row - 1}),
        (row < rows - 2, {"row": row + 2}),
        (row > 1, {"row": row - 2}),
        (col < cols_n - 1, {"col": col + 1}),
        (col > 0, {"col": col - 1}),
    )
    barrier = pltpu.get_barrier_semaphore()
    count = 0
    for there, peer in peers:
        count = count + there.astype(jnp.int32)

        @pl.when(there)
        def _():
            pl.semaphore_signal(barrier, inc=1, device_id=peer, device_id_type=MESH)
    pl.semaphore_wait(barrier, count)

    def copies(g):
        at = pl.ds(pl.multiple_of(g * LANES, LANES), LANES)
        plan = []
        for own, win in ((k_own, win_k), (v_own, win_v)):
            plan += [
                (0, 1, own.at[:, :, at], win.at[g, spill:HALO]),
                (1, 0, own.at[:, :, at], win.at[g, HALO : HALO + depth]),
                (2, 3, own.at[depth - spill : depth, :, at], win.at[g, 0:spill]),
                (3, 2, own.at[0:spill, :, at], win.at[g, HALO + depth : 2 * HALO]),
            ]
        plan += [
            (4, 5, q_ref.at[:, cols - side : cols, at], land_l.at[g]),
            (5, 4, q_ref.at[:, 0:side, at], land_r.at[g]),
        ]
        made = []
        for n, (to, frm, src, dst) in enumerate(plan):
            there, peer = peers[to]
            made.append((there, peers[frm][0], pltpu.make_async_remote_copy(
                src_ref=src, dst_ref=dst, send_sem=send.at[g, n], recv_sem=recv.at[g, n],
                device_id=peer, device_id_type=MESH,
            )))
        return made

    def backs(g):
        made = []
        for n, (to, frm, src, dst) in enumerate(((5, 4, out_l, back_r), (4, 5, out_r, back_l))):
            there, peer = peers[to]
            made.append((there, peers[frm][0], pltpu.make_async_remote_copy(
                src_ref=src.at[g], dst_ref=dst.at[g], send_sem=back_send.at[g, n],
                recv_sem=back_recv.at[g, n], device_id=peer, device_id_type=MESH,
            )))
        return made

    def lses():
        made = []
        for n, (to, frm, src, dst) in enumerate(((5, 4, st_l, lse_r), (4, 5, st_r, lse_l))):
            there, peer = peers[to]
            made.append((there, peers[frm][0], pltpu.make_async_remote_copy(
                src_ref=src, dst_ref=dst, send_sem=back_send.at[groups, n],
                recv_sem=back_recv.at[groups, n], device_id=peer, device_id_type=MESH,
            )))
        return made

    def each(made, which, act):
        for entry in made:
            @pl.when(entry[which])
            def _():
                act(entry[2])

    @pl.loop(0, groups)
    def _(g):
        each(copies(g), 0, lambda copy: copy.start())

    fill_table(cols, 0, 0, WINDOW, tiny[0], x_o, t_o)
    fill_table(side, side, RADIUS_MAX + 1, WINDOW, tiny[1], x_l, t_l)
    fill_table(side, -cols, 0, RADIUS_MAX, tiny[2], x_r, t_r)
    for ref in (l_own, st_l, st_r):
        ref[...] = jnp.zeros_like(ref)
    anchor = row * depth

    @pl.loop(0, groups)
    def _(g):
        at = pl.ds(pl.multiple_of(g * LANES, LANES), LANES)
        each(copies(g), 1, lambda copy: copy.wait_recv())
        for ref, win, own in ((k_ref, win_k, k_own), (v_ref, win_v, v_own)):
            ref[0:HALO] = win[g, 0:HALO]
            ref[HALO : HALO + depth] = own[:, :, at]
            ref[HALO + depth : 2 * HALO + depth] = win[g, HALO : 2 * HALO]
        q_l[...] = land_l[g]
        q_r[...] = land_r[g]

        @pl.when(g > 0)
        def _():
            each(backs(g - 1), 0, lambda copy: copy.start())

        def put_own(slot, value):
            o_own[slot, :, at] = value

        def put_left(slot, value):
            out_l[g, slot] = value

        def put_right(slot, value):
            out_r[g, slot] = value

        @pl.loop(0, BLOCKS)
        def _(beta):
            one_set(tiny[0], anchor, total_rows, g, beta, lambda i: q_ref[i, :, at], t_o, put_own, l_own, k_ref, v_ref, s_o, p_o)
            one_set(tiny[1], anchor, total_rows, g, beta, lambda i: q_l[i], t_l, put_left, st_l, k_ref, v_ref, s_l, p_l)
            one_set(tiny[2], anchor, total_rows, g, beta, lambda i: q_r[i], t_r, put_right, st_r, k_ref, v_ref, s_r, p_r)

    each(backs(groups - 1), 0, lambda copy: copy.start())
    each(lses(), 0, lambda copy: copy.start())

    @pl.loop(0, groups)
    def _(g):
        each(copies(g), 0, lambda copy: copy.wait_send())
        each(backs(g), 0, lambda copy: copy.wait_send())
        each(backs(g), 1, lambda copy: copy.wait_recv())
    each(lses(), 0, lambda copy: copy.wait_send())
    each(lses(), 1, lambda copy: copy.wait_recv())


def window_attention(tiny, total_rows, q, k, v, wide):
    depth, cols, features = q.shape
    groups = features // LANES
    heads = groups * GROUP
    keys = BLOCK_KEYS * 32
    counts = (cols, SIDE_COLS, SIDE_COLS)
    vmem = pl.BlockSpec(memory_space=pltpu.VMEM)
    hbm = pl.BlockSpec(memory_space=pl.ANY)
    bf16, f32 = jnp.bfloat16, jnp.float32
    dma = pltpu.SemaphoreType.DMA
    return pl.pallas_call(
        functools.partial(window_kernel, total_rows, groups),
        in_specs=[pl.BlockSpec(memory_space=pltpu.SMEM)] + [vmem] * 6,
        out_specs=[vmem, vmem, hbm, hbm, hbm, hbm],
        out_shape=[
            jax.ShapeDtypeStruct((SLOTS, cols, features), bf16),
            jax.ShapeDtypeStruct((SLOTS, cols, 128), f32),
            jax.ShapeDtypeStruct((groups, SLOTS, SIDE_COLS, LANES), bf16),
            jax.ShapeDtypeStruct((groups, SLOTS, SIDE_COLS, LANES), bf16),
            jax.ShapeDtypeStruct((SLOTS, SIDE_COLS, 128), f32),
            jax.ShapeDtypeStruct((SLOTS, SIDE_COLS, 128), f32),
        ],
        scratch_shapes=[pltpu.VMEM((groups, 2 * HALO, cols, LANES), bf16)] * 2
        + [pltpu.VMEM((depth + 2 * HALO, cols, LANES), bf16)] * 2
        + [pltpu.VMEM((groups, depth, SIDE_COLS, LANES), bf16)] * 2
        + [pltpu.VMEM((depth, SIDE_COLS, LANES), bf16)] * 2
        + [pltpu.VMEM((heads, BLOCK_ROWS, n, keys), f32) for n in counts]
        + [pltpu.VMEM((GROUP * BLOCK_ROWS * n, keys), f32) for n in counts]
        + [pltpu.VMEM((GROUP * BLOCK_ROWS * n, keys), bf16) for n in counts]
        + [pltpu.VMEM((groups, SLOTS, SIDE_COLS, LANES), bf16)] * 2
        + [pltpu.VMEM((SLOTS, SIDE_COLS, 128), f32)] * 2
        + [dma((groups, 10)), dma((groups, 10)), dma((groups + 1, 2)), dma((groups + 1, 2))],
        compiler_params=pltpu.CompilerParams(
            collective_id=0, has_side_effects=True, vmem_limit_bytes=62 * 2**20
        ),
        cost_estimate=pl.CostEstimate(flops=2 * 10**10, bytes_accessed=4 * 10**7, transcendentals=0),
        name="window_attention",
    )(tiny, q, k, v, *wide)


def merge_kernel(places, slots, flags, own, left, right, l_o, l_l, l_r, w_ref, a_ref, part_ref):
    step = pl.program_id(0)
    rows = 4
    cols = own.shape[1]
    features = own.shape[2]
    groups = left.shape[0]
    pick = lax.broadcasted_iota(jnp.int32, (128, features), 1) // HEAD_DIM
    pick = (pick == lax.broadcasted_iota(jnp.int32, (128, features), 0)).astype(jnp.bfloat16)
    tail = cols - l_l.shape[1]
    has_left, has_right = flags[0] > 0, flags[1] > 0

    def lay(value, ahead, fill):
        blank = jnp.full((tail, value.shape[1]), fill, jnp.float32)
        return jnp.concatenate([blank, value] if ahead else [value, blank], axis=0)

    def whole(ref, slot, there):
        value = jnp.concatenate([ref[g, slot].astype(jnp.float32) for g in range(groups)], axis=1)
        return jnp.where(there, value, 0.0)

    first, second, third = [], [], []
    mine, lefts, rights = [], [], []
    for i in range(rows):
        slot = slots[step * rows + i]
        a = l_o[slot]
        b = jnp.where(has_left, lay(l_l[slot], False, NEG), NEG)
        c = jnp.where(has_right, lay(l_r[slot], True, NEG), NEG)
        top = jnp.maximum(jnp.maximum(a, b), c)
        a, b, c = jnp.exp(a - top), jnp.exp(b - top), jnp.exp(c - top)
        total = a + b + c
        first.append(a / total)
        second.append(b / total)
        third.append(c / total)
        mine.append(own[slot].astype(jnp.float32))
        lefts.append(lay(whole(left, slot, has_left), False, 0.0))
        rights.append(lay(whole(right, slot, has_right), True, 0.0))

    def wide(parts):
        value = jnp.concatenate(parts, axis=0)
        high = value.astype(jnp.bfloat16)
        low = (value - high.astype(jnp.float32)).astype(jnp.bfloat16)
        dot = lambda x: jnp.dot(x, pick, preferred_element_type=jnp.float32)
        return dot(high) + dot(low)

    total = wide(first) * jnp.concatenate(mine, axis=0)
    total = total + wide(second) * jnp.concatenate(lefts, axis=0)
    total = total + wide(third) * jnp.concatenate(rights, axis=0)
    attended = total.astype(jnp.bfloat16)
    a_ref[...] = attended
    part_ref[...] = jnp.dot(attended, w_ref[...], preferred_element_type=jnp.float32).astype(jnp.bfloat16)


def merge(peer, slots, flags, arrays, weight, depth):
    own = arrays[0]
    cols, features = own.shape[1:]
    rows = 4
    half = weight.shape[1] // 2
    full = lambda arr: pl.BlockSpec(arr.shape, lambda i, *_: (0,) * arr.ndim)
    flat = lambda n: pl.BlockSpec((rows * cols, n), lambda i, *_: (i, 0))
    return pl.pallas_call(
        merge_kernel,
        grid_spec=pltpu.PrefetchScalarGridSpec(
            num_scalar_prefetch=3,
            grid=(depth // rows,),
            in_specs=[full(arr) for arr in arrays]
            + [pl.BlockSpec((features, half), lambda i, p, *_: (0, p[0]))],
            out_specs=[flat(features), flat(half)],
        ),
        out_shape=[
            jax.ShapeDtypeStruct((depth * cols, features), jnp.bfloat16),
            jax.ShapeDtypeStruct((depth * cols, half), jnp.bfloat16),
        ],
        compiler_params=pltpu.CompilerParams(vmem_limit_bytes=56 * 2**20),
        cost_estimate=pl.CostEstimate(flops=3 * 10**9, bytes_accessed=2 * 10**7, transcendentals=0),
        name="merge_project",
    )(peer, slots, flags, *arrays, weight)


def shards(query_map, key_map, value_map, window_mask, tile_radius, dilation_per_tile, rel_bias, out_weight):
    depth, cols, features = query_map.shape
    total_rows = depth * lax.axis_size("row")
    settings = jnp.concatenate(
        [window_mask.reshape(-1), tile_radius.reshape(-1), dilation_per_tile.reshape(-1)]
    )
    from_left = shifted(settings, "col", 1)
    from_right = shifted(settings, "col", -1)
    wide = []
    dilations = []
    for values, first, last in (
        (settings, 0, WINDOW),
        (from_left, RADIUS_MAX + 1, WINDOW),
        (from_right, 0, RADIUS_MAX),
    ):
        pattern = values[:-2].reshape(WINDOW, WINDOW)
        dilations.append(jnp.maximum(values[-1], 1))
        wide.append(spread_bias(pattern, values[-2], rel_bias, first, last))
    tiny = jnp.stack(dilations).astype(jnp.int32)
    arrays = window_attention(tiny, total_rows, query_map, key_map, value_map, wide)
    o_own, l_own, back_l, back_r, lse_l, lse_r = arrays
    d = dilations[0]
    index = jnp.arange(depth, dtype=jnp.int32)
    turn = index // d
    slots = (d * (turn // BLOCK_ROWS) + index % d) * BLOCK_ROWS + turn % BLOCK_ROWS
    col = lax.axis_index("col")
    head = lax.axis_index("head")
    flags = jnp.stack([col > 0, col < lax.axis_size("col") - 1]).astype(jnp.int32)
    attended, theirs = merge(
        (1 - head).astype(jnp.int32).reshape(1), slots.astype(jnp.int32), flags,
        (o_own, back_l, back_r, l_own, lse_l, lse_r), out_weight, depth,
    )
    arrived = lax.ppermute(theirs, "head", [(0, 1), (1, 0)])
    half = out_weight.shape[1] // 2
    my_weight = lax.dynamic_slice_in_dim(out_weight, head * half, half, 1)
    mine = jnp.dot(attended, my_weight, preferred_element_type=jnp.float32)
    mine, arrived = lax.optimization_barrier((mine, arrived))
    return (mine + arrived.astype(jnp.float32)).astype(jnp.bfloat16).reshape(depth, cols, half)


def solution(mesh):
    placed = (
        P("row", "col", "head"),
        P("row", "col", "head"),
        P("row", "col", "head"),
        P("row", "col", None, None),
        P("row", "col"),
        P("row", "col"),
        P("head", None, None),
        P("head", None),
    )
    return jax.shard_map(
        shards, mesh=mesh, in_specs=placed, out_specs=P("row", "col", "head"), check_vma=False
    )
```

```python
import functools

import jax
import jax.numpy as jnp
from jax import lax
from jax.experimental import pallas as pl
from jax.experimental.pallas import tpu as pltpu
from jax.sharding import PartitionSpec as P

HEAD_DIM = 64
RADIUS_MAX = 6
WINDOW = 13
HALO = 18
NEG = -1e30
BLOCK_ROWS = 3
BLOCK_KEYS = 16
SIDE_COLS = 24
GROUP = 4
LANES = GROUP * HEAD_DIM
BLOCKS = 6
SLOTS = BLOCKS * BLOCK_ROWS


MESH = pl.DeviceIdType.MESH


def shifted(value, axis, steps):
    count = lax.axis_size(axis)
    leading, last = (max(0, -steps), min(count, count - steps))
    return lax.ppermute(value, axis, [(source, source + steps) for source in range(leading, last)])


def spread_bias(pattern, radius, rel_bias, first, last):
    heads = rel_bias.shape[0]
    steps = jnp.abs(jnp.arange(WINDOW, dtype=jnp.int32) - RADIUS_MAX)
    centre = (steps[:, None] == 0) & (steps[None, :] == 0)
    near = (steps[:, None] <= radius) & (steps[None, :] <= radius)
    used = ((pattern == 1) | centre) & near
    masked = jnp.where(used[None], rel_bias, NEG)
    turned = jnp.swapaxes(masked, 1, 2)[:, first:last]
    extra = BLOCK_KEYS - WINDOW
    turned = jnp.pad(turned, ((0, 0), (0, 0), (BLOCK_ROWS - 1, extra)), constant_values=NEG)
    parts = [turned[:, :, BLOCK_ROWS - 1 - t :][:, :, :BLOCK_KEYS] for t in range(BLOCK_ROWS)]
    count = BLOCK_ROWS * (last - first)
    flat = jnp.stack(parts, axis=1).reshape(heads, count, BLOCK_KEYS)
    flat = jnp.pad(flat, ((0, 0), (0, -count % 8), (0, 0)), constant_values=NEG)
    return flat.reshape(-1, BLOCK_KEYS)


def expand_bias(flat_ref, x_ref):
    value = flat_ref[...]
    high = value.astype(jnp.bfloat16)
    rest = value - high.astype(jnp.float32)
    middle = rest.astype(jnp.bfloat16)
    low = (rest - middle.astype(jnp.float32)).astype(jnp.bfloat16)
    width = x_ref.shape[1]
    pick = lax.broadcasted_iota(jnp.int32, (BLOCK_KEYS, width), 1) // 32
    pick = (pick == lax.broadcasted_iota(jnp.int32, (BLOCK_KEYS, width), 0)).astype(jnp.bfloat16)
    dot = lambda part: jnp.dot(part, pick, preferred_element_type=jnp.float32)
    x_ref[...] = dot(high) + dot(middle) + dot(low)


def fill_table(offset, first, last, d, x_ref, t_ref):
    heads, _, cols, width = t_ref.shape
    stride = x_ref.shape[0] // heads
    count = last - first

    @pl.loop(0, heads)
    def _(h):
        rows = x_ref[pl.ds(pl.multiple_of(h * stride, 8), stride)]
        for top in range(0, cols, 8):
            lane = lax.broadcasted_iota(jnp.int32, (8, 128), 1)
            rel = lane % 32 - lax.broadcasted_iota(jnp.int32, (8, 128), 0) + (offset - top)
            masks = [rel == (b + first - RADIUS_MAX) * d for b in range(count)]
            for t in range(BLOCK_ROWS):
                for left in range(0, width, 128):
                    acc = jnp.full((8, 128), NEG, jnp.float32)
                    for b in range(count):
                        at = t * count + b
                        acc = jnp.where(masks[b], rows[at : at + 1, left : left + 128], acc)
                    t_ref[h, t, top : top + 8, left : left + 128] = acc


def base_row(beta, d):
    two = beta % 2 + 6 * (beta // 2)
    three = beta % 3 + 9 * (beta // 3)
    return jnp.where(d == 1, 3 * beta, jnp.where(d == 2, two, three))


def one_set(d, row_anchor, total_rows, group, beta, load_q, t_ref, store_o, l_ref, k_ref, v_ref, s_ref, p_ref):
    cols = t_ref.shape[2]
    base = base_row(beta, d)
    span = k_ref.shape[0]
    depth = span - 2 * HALO
    width = BLOCK_KEYS * 32
    queries = []
    for t in range(BLOCK_ROWS):
        row = jnp.minimum(base + t * d, depth - 1)
        queries.append(load_q(row).astype(jnp.float32) * 0.125)
    queries = jnp.concatenate(queries, axis=0)
    lane_head = lax.broadcasted_iota(jnp.int32, queries.shape, 1) // HEAD_DIM
    spread = [jnp.where(lane_head == h, queries, 0.0) for h in range(GROUP)]
    spread = jnp.concatenate(spread, axis=0).astype(jnp.bfloat16)
    key_rows = []
    value_rows = []
    for u in range(BLOCK_KEYS):
        row = jnp.clip(HALO + base + (u - RADIUS_MAX) * d, 0, span - 1)
        key_rows.append(k_ref[row])
        value_rows.append(v_ref[row])
    keys = jnp.concatenate(key_rows, axis=0)
    values = jnp.concatenate(value_rows, axis=0)
    s_ref[...] = lax.dot_general(
        spread, keys, (((1,), (1,)), ((), ())), preferred_element_type=jnp.float32
    )
    step = lax.broadcasted_iota(jnp.int32, (1, width), 1) // 32
    key_row = row_anchor + base + (step - RADIUS_MAX) * d
    row_bias = jnp.where((key_row >= 0) & (key_row < total_rows), 0.0, NEG)
    sums = []
    peaks = []
    for h in range(GROUP):
        for t in range(BLOCK_ROWS):
            at = (h * BLOCK_ROWS + t) * cols
            score = s_ref[at : at + cols] + (t_ref[group * GROUP + h, t] + row_bias)
            peak = jnp.maximum(jnp.max(score, axis=1, keepdims=True), -1e20)
            weight = jnp.exp(score - peak)
            sums.append(jnp.sum(weight, axis=1, keepdims=True))
            peaks.append(peak)
            p_ref[at : at + cols] = weight.astype(jnp.bfloat16)
    mixed = jnp.dot(p_ref[...], values, preferred_element_type=jnp.float32)
    head_of = lax.broadcasted_iota(jnp.int32, (cols, LANES), 1) // HEAD_DIM
    stat_lane = lax.broadcasted_iota(jnp.int32, (cols, 128), 1)
    for t in range(BLOCK_ROWS):
        slot = beta * BLOCK_ROWS + t
        out = jnp.zeros((cols, LANES), jnp.float32)
        stats = l_ref[slot]
        for h in range(GROUP):
            at = h * BLOCK_ROWS + t
            total = sums[at]
            some = total > 0.0
            inverse = 1.0 / jnp.where(some, total, 1.0)
            out = jnp.where(head_of == h, mixed[at * cols : (at + 1) * cols] * inverse, out)
            lse = jnp.where(some, peaks[at] + jnp.log(jnp.where(some, total, 1.0)), NEG)
            stats = jnp.where(stat_lane == group * GROUP + h, lse, stats)
        store_o(slot, out.astype(jnp.bfloat16))
        l_ref[slot] = stats


def merge_rows(step, rows, slots, has_left, has_right, own, left, right, l_o, l_l, l_r):
    cols, features = own.shape[1:]
    groups = left.shape[0]
    pick = lax.broadcasted_iota(jnp.int32, (128, features), 1) // HEAD_DIM
    pick = (pick == lax.broadcasted_iota(jnp.int32, (128, features), 0)).astype(jnp.bfloat16)
    tail = cols - l_l.shape[1]

    def lay(value, ahead, fill):
        blank = jnp.full((tail, value.shape[1]), fill, jnp.float32)
        return jnp.concatenate([blank, value] if ahead else [value, blank], axis=0)

    def whole(ref, slot, there):
        value = jnp.concatenate([ref[g, slot].astype(jnp.float32) for g in range(groups)], axis=1)
        return jnp.where(there, value, 0.0)

    first, second, third = [], [], []
    mine, lefts, rights = [], [], []
    for i in range(rows):
        slot = slots[step * rows + i]
        a = l_o[slot]
        b = jnp.where(has_left, lay(l_l[slot], False, NEG), NEG)
        c = jnp.where(has_right, lay(l_r[slot], True, NEG), NEG)
        top = jnp.maximum(jnp.maximum(a, b), c)
        a, b, c = jnp.exp(a - top), jnp.exp(b - top), jnp.exp(c - top)
        total = a + b + c
        first.append(a / total)
        second.append(b / total)
        third.append(c / total)
        mine.append(own[slot].astype(jnp.float32))
        lefts.append(lay(whole(left, slot, has_left), False, 0.0))
        rights.append(lay(whole(right, slot, has_right), True, 0.0))

    def wide(parts):
        value = jnp.concatenate(parts, axis=0)
        high = value.astype(jnp.bfloat16)
        low = (value - high.astype(jnp.float32)).astype(jnp.bfloat16)
        dot = lambda x: jnp.dot(x, pick, preferred_element_type=jnp.float32)
        return dot(high) + dot(low)

    total = wide(first) * jnp.concatenate(mine, axis=0)
    total = total + wide(second) * jnp.concatenate(lefts, axis=0)
    total = total + wide(third) * jnp.concatenate(rights, axis=0)
    return total.astype(jnp.bfloat16)


def window_kernel(
    total_rows, groups, tiny, slots, q_ref, k_own, v_own, flat_o, flat_l, flat_r, w_hbm,
    result,
    o_own, l_own, back_l, back_r, lse_l, lse_r, w_theirs, w_mine, attended, parts, arrived, x_o, x_l, x_r,
    win_k, win_v, k_ref, v_ref, land_l, land_r, q_l, q_r, t_o, t_l, t_r,
    s_o, s_l, s_r, p_o, p_l, p_r, out_l, out_r, st_l, st_r,
    send, recv, back_send, back_recv, head_send, head_recv, w_sem,
):
    row, col, head = lax.axis_index("row"), lax.axis_index("col"), lax.axis_index("head")
    rows, cols_n = lax.axis_size("row"), lax.axis_size("col")
    depth, cols, _ = k_own.shape
    spill = HALO - depth
    side = land_l.shape[2]
    half = w_mine.shape[1]
    weights = [
        pltpu.make_async_copy(w_hbm.at[:, pl.ds(pl.multiple_of(which * half, 128), half)], dst, w_sem.at[n])
        for n, (which, dst) in enumerate(((1 - head, w_theirs), (head, w_mine)))
    ]

    for edge, at, n in (
        (row < 2, 0, spill),
        (row < 1, spill, depth),
        (row > rows - 2, HALO, depth),
        (row > rows - 3, HALO + depth, spill),
    ):
        @pl.when(edge)
        def _():
            for ref in (win_k, win_v):
                ref[:, at : at + n] = jnp.zeros((groups, n, cols, LANES), ref.dtype)
    for edge, ref in ((col < 1, land_l), (col > cols_n - 2, land_r)):
        @pl.when(edge)
        def _():
            ref[...] = jnp.zeros_like(ref)

    peers = (
        (row < rows - 1, {"row": row + 1}),
        (row > 0, {"row": row - 1}),
        (row < rows - 2, {"row": row + 2}),
        (row > 1, {"row": row - 2}),
        (col < cols_n - 1, {"col": col + 1}),
        (col > 0, {"col": col - 1}),
    )
    barrier = pltpu.get_barrier_semaphore()
    pl.semaphore_signal(barrier, inc=1, device_id={"head": 1 - head}, device_id_type=MESH)
    count = 1
    for there, peer in peers:
        count = count + there.astype(jnp.int32)

        @pl.when(there)
        def _():
            pl.semaphore_signal(barrier, inc=1, device_id=peer, device_id_type=MESH)
    pl.semaphore_wait(barrier, count)

    def copies(g):
        at = pl.ds(pl.multiple_of(g * LANES, LANES), LANES)
        plan = []
        for own, win in ((k_own, win_k), (v_own, win_v)):
            plan += [
                (0, 1, own.at[:, :, at], win.at[g, spill:HALO]),
                (1, 0, own.at[:, :, at], win.at[g, HALO : HALO + depth]),
                (2, 3, own.at[depth - spill : depth, :, at], win.at[g, 0:spill]),
                (3, 2, own.at[0:spill, :, at], win.at[g, HALO + depth : 2 * HALO]),
            ]
        plan += [
            (4, 5, q_ref.at[:, cols - side : cols, at], land_l.at[g]),
            (5, 4, q_ref.at[:, 0:side, at], land_r.at[g]),
        ]
        made = []
        for n, (to, frm, src, dst) in enumerate(plan):
            there, peer = peers[to]
            made.append((there, peers[frm][0], pltpu.make_async_remote_copy(
                src_ref=src, dst_ref=dst, send_sem=send.at[g, n], recv_sem=recv.at[g, n],
                device_id=peer, device_id_type=MESH,
            )))
        return made

    def backs(g):
        made = []
        for n, (to, frm, src, dst) in enumerate(((5, 4, out_l, back_r), (4, 5, out_r, back_l))):
            there, peer = peers[to]
            made.append((there, peers[frm][0], pltpu.make_async_remote_copy(
                src_ref=src.at[g], dst_ref=dst.at[g], send_sem=back_send.at[g, n],
                recv_sem=back_recv.at[g, n], device_id=peer, device_id_type=MESH,
            )))
        return made

    def lses():
        made = []
        for n, (to, frm, src, dst) in enumerate(((5, 4, st_l, lse_r), (4, 5, st_r, lse_l))):
            there, peer = peers[to]
            made.append((there, peers[frm][0], pltpu.make_async_remote_copy(
                src_ref=src, dst_ref=dst, send_sem=back_send.at[groups, n],
                recv_sem=back_recv.at[groups, n], device_id=peer, device_id_type=MESH,
            )))
        return made

    def each(made, which, act):
        for entry in made:
            @pl.when(entry[which])
            def _():
                act(entry[2])

    @pl.loop(0, groups)
    def _(g):
        each(copies(g), 0, lambda copy: copy.start())

    for copy in weights:
        copy.start()
    for flat, wide in ((flat_o, x_o), (flat_l, x_l), (flat_r, x_r)):
        expand_bias(flat, wide)
    fill_table(0, 0, WINDOW, tiny[0], x_o, t_o)
    fill_table(side, RADIUS_MAX + 1, WINDOW, tiny[1], x_l, t_l)
    fill_table(-cols, 0, RADIUS_MAX, tiny[2], x_r, t_r)
    for ref in (l_own, st_l, st_r):
        ref[...] = jnp.zeros_like(ref)
    anchor = row * depth

    @pl.loop(0, groups)
    def _(g):
        at = pl.ds(pl.multiple_of(g * LANES, LANES), LANES)
        each(copies(g), 1, lambda copy: copy.wait_recv())
        for ref, win, own in ((k_ref, win_k, k_own), (v_ref, win_v, v_own)):
            ref[0:HALO] = win[g, 0:HALO]
            ref[HALO : HALO + depth] = own[:, :, at]
            ref[HALO + depth : 2 * HALO + depth] = win[g, HALO : 2 * HALO]
        q_l[...] = land_l[g]
        q_r[...] = land_r[g]

        @pl.when(g > 0)
        def _():
            each(backs(g - 1), 0, lambda copy: copy.start())

        def put_own(slot, value):
            o_own[slot, :, at] = value

        def put_left(slot, value):
            out_l[g, slot] = value

        def put_right(slot, value):
            out_r[g, slot] = value

        @pl.loop(0, BLOCKS)
        def _(beta):
            one_set(tiny[0], anchor, total_rows, g, beta, lambda i: q_ref[i, :, at], t_o, put_own, l_own, k_ref, v_ref, s_o, p_o)
            one_set(tiny[1], anchor, total_rows, g, beta, lambda i: q_l[i], t_l, put_left, st_l, k_ref, v_ref, s_l, p_l)
            one_set(tiny[2], anchor, total_rows, g, beta, lambda i: q_r[i], t_r, put_right, st_r, k_ref, v_ref, s_r, p_r)

    for copy in weights:
        copy.wait()

    @pl.loop(0, groups)
    def _(g):
        each(copies(g), 0, lambda copy: copy.wait_send())

    each(backs(groups - 1), 0, lambda copy: copy.start())
    each(lses(), 0, lambda copy: copy.start())

    @pl.loop(0, groups)
    def _(g):
        each(backs(g), 1, lambda copy: copy.wait_recv())

    each(lses(), 1, lambda copy: copy.wait_recv())

    def swap(i):
        return pltpu.make_async_remote_copy(
            src_ref=parts.at[i], dst_ref=arrived.at[i], send_sem=head_send.at[i], recv_sem=head_recv.at[i],
            device_id={"head": 1 - head}, device_id_type=MESH,
        )

    steps = parts.shape[0]

    @pl.loop(0, steps)
    def _(i):
        attended[i] = merge_rows(
            i, depth // steps, slots, col > 0, col < cols_n - 1, o_own, back_l, back_r, l_own, lse_l, lse_r
        )

        @pl.when(i > 0)
        def _():
            swap(i - 1).start()

        parts[i] = jnp.dot(attended[i], w_theirs[...], preferred_element_type=jnp.float32).astype(jnp.bfloat16)

    @pl.loop(0, groups)
    def _(g):
        each(backs(g), 0, lambda copy: copy.wait_send())

    each(lses(), 0, lambda copy: copy.wait_send())
    swap(steps - 1).start()

    @pl.loop(0, steps)
    def _(i):
        mine = jnp.dot(attended[i], w_mine[...], preferred_element_type=jnp.float32)
        swap(i).wait_recv()
        result[i] = (mine + arrived[i].astype(jnp.float32)).astype(jnp.bfloat16)

    @pl.loop(0, steps)
    def _(i):
        swap(i).wait_send()


def window_attention(tiny, slots, total_rows, q, k, v, flats, weight):
    depth, cols, features = q.shape
    groups = features // LANES
    heads = groups * GROUP
    keys = BLOCK_KEYS * 32
    half = weight.shape[1] // 2
    steps = 4
    tokens = depth * cols // steps
    counts = (cols, SIDE_COLS, SIDE_COLS)
    vmem = pl.BlockSpec(memory_space=pltpu.VMEM)
    smem = pl.BlockSpec(memory_space=pltpu.SMEM)
    bf16, f32 = jnp.bfloat16, jnp.float32
    dma = pltpu.SemaphoreType.DMA
    return pl.pallas_call(
        functools.partial(window_kernel, total_rows, groups),
        in_specs=[smem, smem] + [vmem] * 6 + [pl.BlockSpec(memory_space=pl.ANY)],
        out_specs=vmem,
        out_shape=jax.ShapeDtypeStruct((steps, tokens, half), bf16),
        scratch_shapes=[
            pltpu.VMEM((SLOTS, cols, features), bf16),
            pltpu.VMEM((SLOTS, cols, 128), f32),
            pltpu.VMEM((groups, SLOTS, SIDE_COLS, LANES), bf16),
            pltpu.VMEM((groups, SLOTS, SIDE_COLS, LANES), bf16),
            pltpu.VMEM((SLOTS, SIDE_COLS, 128), f32),
            pltpu.VMEM((SLOTS, SIDE_COLS, 128), f32),
            pltpu.VMEM((features, half), bf16),
            pltpu.VMEM((features, half), bf16),
            pltpu.VMEM((steps, tokens, features), bf16),
            pltpu.VMEM((steps, tokens, half), bf16),
            pltpu.VMEM((steps, tokens, half), bf16),
        ]
        + [pltpu.VMEM((flat.shape[0], keys), f32) for flat in flats]
        + [pltpu.VMEM((groups, 2 * HALO, cols, LANES), bf16)] * 2
        + [pltpu.VMEM((depth + 2 * HALO, cols, LANES), bf16)] * 2
        + [pltpu.VMEM((groups, depth, SIDE_COLS, LANES), bf16)] * 2
        + [pltpu.VMEM((depth, SIDE_COLS, LANES), bf16)] * 2
        + [pltpu.VMEM((heads, BLOCK_ROWS, n, keys), f32) for n in counts]
        + [pltpu.VMEM((GROUP * BLOCK_ROWS * n, keys), f32) for n in counts]
        + [pltpu.VMEM((GROUP * BLOCK_ROWS * n, keys), bf16) for n in counts]
        + [pltpu.VMEM((groups, SLOTS, SIDE_COLS, LANES), bf16)] * 2
        + [pltpu.VMEM((SLOTS, SIDE_COLS, 128), f32)] * 2
        + [dma((groups, 10)), dma((groups, 10)), dma((groups + 1, 2)), dma((groups + 1, 2))]
        + [dma((steps,)), dma((steps,)), dma((2,))],
        compiler_params=pltpu.CompilerParams(
            collective_id=0, has_side_effects=True, vmem_limit_bytes=67_000_000
        ),
        cost_estimate=pl.CostEstimate(flops=2 * 10**10, bytes_accessed=4 * 10**7, transcendentals=0),
        name="window_attention",
    )(tiny, slots, q, k, v, *flats, weight)


def shards(query_map, key_map, value_map, window_mask, tile_radius, dilation_per_tile, rel_bias, out_weight):
    depth, cols, features = query_map.shape
    total_rows = depth * lax.axis_size("row")
    settings = jnp.concatenate(
        [window_mask.reshape(-1), tile_radius.reshape(-1), dilation_per_tile.reshape(-1)]
    )
    from_left = shifted(settings, "col", 1)
    from_right = shifted(settings, "col", -1)
    wide = []
    dilations = []
    for values, first, last in (
        (settings, 0, WINDOW),
        (from_left, RADIUS_MAX + 1, WINDOW),
        (from_right, 0, RADIUS_MAX),
    ):
        pattern = values[:-2].reshape(WINDOW, WINDOW)
        dilations.append(jnp.maximum(values[-1], 1))
        wide.append(spread_bias(pattern, values[-2], rel_bias, first, last))
    tiny = jnp.stack(dilations).astype(jnp.int32)
    d = dilations[0]
    index = jnp.arange(depth, dtype=jnp.int32)
    turn = index // d
    slots = (d * (turn // BLOCK_ROWS) + index % d) * BLOCK_ROWS + turn % BLOCK_ROWS
    out = window_attention(
        tiny, slots.astype(jnp.int32), total_rows, query_map, key_map, value_map, wide, out_weight
    )
    return out.reshape(depth, cols, out.shape[2])


def solution(mesh):
    placed = (
        P("row", "col", "head"),
        P("row", "col", "head"),
        P("row", "col", "head"),
        P("row", "col", None, None),
        P("row", "col"),
        P("row", "col"),
        P("head", None, None),
        P("head", None),
    )
    return jax.shard_map(
        shards, mesh=mesh, in_specs=placed, out_specs=P("row", "col", "head"), check_vma=False
    )
```

```python
import functools

import jax
import jax.numpy as jnp
from jax import lax
from jax.experimental import pallas as pl
from jax.experimental.pallas import tpu as pltpu
from jax.sharding import PartitionSpec as P

HEAD_DIM = 64
RADIUS_MAX = 6
WINDOW = 13
HALO = 18
NEG = -1e30
BLOCK_ROWS = 3
BLOCK_KEYS = 16
SIDE_COLS = 24
GROUP = 4
LANES = GROUP * HEAD_DIM
BLOCKS = 6
SLOTS = BLOCKS * BLOCK_ROWS


MESH = pl.DeviceIdType.MESH


def shifted(value, axis, steps):
    count = lax.axis_size(axis)
    leading, last = (max(0, -steps), min(count, count - steps))
    return lax.ppermute(value, axis, [(source, source + steps) for source in range(leading, last)])


def block_form(value, first, last, fill):
    turned = jnp.swapaxes(value, 1, 2)[:, first:last]
    extra = BLOCK_KEYS - WINDOW
    turned = jnp.pad(turned, ((0, 0), (0, 0), (BLOCK_ROWS - 1, extra)), constant_values=fill)
    parts = [turned[:, :, BLOCK_ROWS - 1 - t :][:, :, :BLOCK_KEYS] for t in range(BLOCK_ROWS)]
    count = BLOCK_ROWS * (last - first)
    flat = jnp.stack(parts, axis=1).reshape(value.shape[0], count, BLOCK_KEYS)
    return jnp.pad(flat, ((0, 0), (0, -count % 8), (0, 0)), constant_values=fill)


def expand_bias(flat_ref, mask_ref, x_ref):
    value = (flat_ref[...] + mask_ref[...][None]).reshape(x_ref.shape[0], BLOCK_KEYS)
    high = value.astype(jnp.bfloat16)
    rest = value - high.astype(jnp.float32)
    middle = rest.astype(jnp.bfloat16)
    low = (rest - middle.astype(jnp.float32)).astype(jnp.bfloat16)
    width = x_ref.shape[1]
    pick = lax.broadcasted_iota(jnp.int32, (BLOCK_KEYS, width), 1) // 32
    pick = (pick == lax.broadcasted_iota(jnp.int32, (BLOCK_KEYS, width), 0)).astype(jnp.bfloat16)
    dot = lambda part: jnp.dot(part, pick, preferred_element_type=jnp.float32)
    x_ref[...] = dot(high) + dot(middle) + dot(low)


def fill_table(offset, first, last, d, x_ref, t_ref):
    heads, _, cols, width = t_ref.shape
    stride = x_ref.shape[0] // heads
    count = last - first

    @pl.loop(0, heads)
    def _(h):
        rows = x_ref[pl.ds(pl.multiple_of(h * stride, 8), stride)]
        for top in range(0, cols, 8):
            lane = lax.broadcasted_iota(jnp.int32, (8, 128), 1)
            rel = lane % 32 - lax.broadcasted_iota(jnp.int32, (8, 128), 0) + (offset - top)
            masks = [rel == (b + first - RADIUS_MAX) * d for b in range(count)]
            for t in range(BLOCK_ROWS):
                for left in range(0, width, 128):
                    acc = jnp.full((8, 128), NEG, jnp.float32)
                    for b in range(count):
                        at = t * count + b
                        acc = jnp.where(masks[b], rows[at : at + 1, left : left + 128], acc)
                    t_ref[h, t, top : top + 8, left : left + 128] = acc


def base_row(beta, d):
    two = beta % 2 + 6 * (beta // 2)
    three = beta % 3 + 9 * (beta // 3)
    return jnp.where(d == 1, 3 * beta, jnp.where(d == 2, two, three))


def one_set(d, row_anchor, total_rows, group, beta, load_q, t_ref, store_o, load_l, store_l, k_ref, v_ref, s_ref, p_ref):
    cols = t_ref.shape[2]
    base = base_row(beta, d)
    span = k_ref.shape[0]
    depth = span - 2 * HALO
    width = BLOCK_KEYS * 32
    queries = []
    for t in range(BLOCK_ROWS):
        row = jnp.minimum(base + t * d, depth - 1)
        queries.append(load_q(row).astype(jnp.float32) * 0.125)
    queries = jnp.concatenate(queries, axis=0)
    lane_head = lax.broadcasted_iota(jnp.int32, queries.shape, 1) // HEAD_DIM
    spread = [jnp.where(lane_head == h, queries, 0.0) for h in range(GROUP)]
    spread = jnp.concatenate(spread, axis=0).astype(jnp.bfloat16)
    key_rows = []
    value_rows = []
    for u in range(BLOCK_KEYS):
        row = jnp.clip(HALO + base + (u - RADIUS_MAX) * d, 0, span - 1)
        key_rows.append(k_ref[row])
        value_rows.append(v_ref[row])
    keys = jnp.concatenate(key_rows, axis=0)
    values = jnp.concatenate(value_rows, axis=0)
    s_ref[...] = lax.dot_general(
        spread, keys, (((1,), (1,)), ((), ())), preferred_element_type=jnp.float32
    )
    step = lax.broadcasted_iota(jnp.int32, (1, width), 1) // 32
    key_row = row_anchor + base + (step - RADIUS_MAX) * d
    row_bias = jnp.where((key_row >= 0) & (key_row < total_rows), 0.0, NEG)
    sums = []
    peaks = []
    for h in range(GROUP):
        for t in range(BLOCK_ROWS):
            at = (h * BLOCK_ROWS + t) * cols
            score = s_ref[at : at + cols] + (t_ref[group * GROUP + h, t] + row_bias)
            peak = jnp.maximum(jnp.max(score, axis=1, keepdims=True), -1e20)
            weight = jnp.exp(score - peak)
            sums.append(jnp.sum(weight, axis=1, keepdims=True))
            peaks.append(peak)
            p_ref[at : at + cols] = weight.astype(jnp.bfloat16)
    mixed = jnp.dot(p_ref[...], values, preferred_element_type=jnp.float32)
    head_of = lax.broadcasted_iota(jnp.int32, (cols, LANES), 1) // HEAD_DIM
    stat_lane = lax.broadcasted_iota(jnp.int32, (cols, 128), 1)
    for t in range(BLOCK_ROWS):
        slot = beta * BLOCK_ROWS + t
        out = jnp.zeros((cols, LANES), jnp.float32)
        stats, lane0 = load_l(slot)
        for h in range(GROUP):
            at = h * BLOCK_ROWS + t
            total = sums[at]
            some = total > 0.0
            inverse = 1.0 / jnp.where(some, total, 1.0)
            out = jnp.where(head_of == h, mixed[at * cols : (at + 1) * cols] * inverse, out)
            lse = jnp.where(some, peaks[at] + jnp.log(jnp.where(some, total, 1.0)), NEG)
            stats = jnp.where(stat_lane == lane0 + h, lse, stats)
        store_o(slot, out.astype(jnp.bfloat16))
        store_l(slot, stats)


def merge_rows(step, rows, slots, has_left, has_right, own, left, right, l_o, l_l, l_r):
    cols, features = own.shape[1:]
    groups = left.shape[0]
    pick = lax.broadcasted_iota(jnp.int32, (128, features), 1) // HEAD_DIM
    pick = (pick == lax.broadcasted_iota(jnp.int32, (128, features), 0)).astype(jnp.bfloat16)
    tail = cols - l_l.shape[1]

    def found(ref, slot):
        lane = lax.broadcasted_iota(jnp.int32, (cols - tail, 128), 1)
        value = jnp.full((cols - tail, 128), NEG, jnp.float32)
        for g in range(groups):
            packed = ref[g]
            for h in range(GROUP):
                one = jnp.sum(jnp.where(lane == slot * GROUP + h, packed, 0.0), axis=1, keepdims=True)
                value = jnp.where(lane == g * GROUP + h, one, value)
        return value

    def lay(value, ahead, fill):
        blank = jnp.full((tail, value.shape[1]), fill, jnp.float32)
        return jnp.concatenate([blank, value] if ahead else [value, blank], axis=0)

    def whole(ref, slot, there):
        value = jnp.concatenate([ref[g, slot].astype(jnp.float32) for g in range(groups)], axis=1)
        return jnp.where(there, value, 0.0)

    first, second, third = [], [], []
    mine, lefts, rights = [], [], []
    for i in range(rows):
        slot = slots[step * rows + i]
        a = l_o[slot]
        b = jnp.where(has_left, lay(found(l_l, slot), False, NEG), NEG)
        c = jnp.where(has_right, lay(found(l_r, slot), True, NEG), NEG)
        top = jnp.maximum(jnp.maximum(a, b), c)
        a, b, c = jnp.exp(a - top), jnp.exp(b - top), jnp.exp(c - top)
        total = a + b + c
        first.append(a / total)
        second.append(b / total)
        third.append(c / total)
        mine.append(own[slot].astype(jnp.float32))
        lefts.append(lay(whole(left, slot, has_left), False, 0.0))
        rights.append(lay(whole(right, slot, has_right), True, 0.0))

    def wide(parts):
        value = jnp.concatenate(parts, axis=0)
        high = value.astype(jnp.bfloat16)
        low = (value - high.astype(jnp.float32)).astype(jnp.bfloat16)
        dot = lambda x: jnp.dot(x, pick, preferred_element_type=jnp.float32)
        return dot(high) + dot(low)

    total = wide(first) * jnp.concatenate(mine, axis=0)
    total = total + wide(second) * jnp.concatenate(lefts, axis=0)
    total = total + wide(third) * jnp.concatenate(rights, axis=0)
    return total.astype(jnp.bfloat16)


def window_kernel(
    total_rows, groups, d_own, slots, q_ref, k_own, v_own, flat_o, flat_l, flat_r, m_o, m_right, m_left, w_hbm,
    result,
    o_own, l_own, back_l, back_r, lse_l, lse_r, w_theirs, w_mine, attended, parts, arrived, x_o, x_l, x_r,
    win_k, win_v, k_ref, v_ref, land_l, land_r, q_l, q_r, t_o, t_l, t_r,
    s_o, s_l, s_r, p_o, p_l, p_r, out_l, out_r, st_l, st_r,
    send, recv, back_send, back_recv, head_send, head_recv, w_sem, m_l, m_r, d_l, d_r, set_send, set_recv,
):
    row, col, head = lax.axis_index("row"), lax.axis_index("col"), lax.axis_index("head")
    rows, cols_n = lax.axis_size("row"), lax.axis_size("col")
    depth, cols, _ = k_own.shape
    spill = HALO - depth
    side = land_l.shape[2]
    half = w_mine.shape[1]
    weights = [
        pltpu.make_async_copy(w_hbm.at[:, pl.ds(pl.multiple_of(which * half, 128), half)], dst, w_sem.at[n])
        for n, (which, dst) in enumerate(((1 - head, w_theirs), (head, w_mine)))
    ]

    for edge, at, n in (
        (row < 2, 0, spill),
        (row < 1, spill, depth),
        (row > rows - 2, HALO, depth),
        (row > rows - 3, HALO + depth, spill),
    ):
        @pl.when(edge)
        def _():
            for ref in (win_k, win_v):
                ref[:, at : at + n] = jnp.zeros((groups, n, cols, LANES), ref.dtype)
    for edge, ref, mask, d_ref in ((col < 1, land_l, m_l, d_l), (col > cols_n - 2, land_r, m_r, d_r)):
        @pl.when(edge)
        def _():
            ref[...] = jnp.zeros_like(ref)
            mask[...] = jnp.full(mask.shape, NEG, jnp.float32)
            for n in range(d_ref.shape[0]):
                d_ref[n] = 1

    peers = (
        (row < rows - 1, {"row": row + 1}),
        (row > 0, {"row": row - 1}),
        (row < rows - 2, {"row": row + 2}),
        (row > 1, {"row": row - 2}),
        (col < cols_n - 1, {"col": col + 1}),
        (col > 0, {"col": col - 1}),
    )
    barrier = pltpu.get_barrier_semaphore()
    pl.semaphore_signal(barrier, inc=1, device_id={"head": 1 - head}, device_id_type=MESH)
    count = 1
    for there, peer in peers:
        count = count + there.astype(jnp.int32)

        @pl.when(there)
        def _():
            pl.semaphore_signal(barrier, inc=1, device_id=peer, device_id_type=MESH)
    pl.semaphore_wait(barrier, count)

    def copies(g):
        at = pl.ds(pl.multiple_of(g * LANES, LANES), LANES)
        plan = []
        for own, win in ((k_own, win_k), (v_own, win_v)):
            plan += [
                (0, 1, own.at[:, :, at], win.at[g, spill:HALO]),
                (1, 0, own.at[:, :, at], win.at[g, HALO : HALO + depth]),
                (2, 3, own.at[depth - spill : depth, :, at], win.at[g, 0:spill]),
                (3, 2, own.at[0:spill, :, at], win.at[g, HALO + depth : 2 * HALO]),
            ]
        plan += [
            (4, 5, q_ref.at[:, cols - side : cols, at], land_l.at[g]),
            (5, 4, q_ref.at[:, 0:side, at], land_r.at[g]),
        ]
        made = []
        for n, (to, frm, src, dst) in enumerate(plan):
            there, peer = peers[to]
            made.append((there, peers[frm][0], pltpu.make_async_remote_copy(
                src_ref=src, dst_ref=dst, send_sem=send.at[g, n], recv_sem=recv.at[g, n],
                device_id=peer, device_id_type=MESH,
            )))
        return made

    per = SLOTS // 2

    def backs(k):
        g, at = k // 2, pl.ds((k % 2) * per, per)
        made = []
        for n, (to, frm, src, dst) in enumerate(((5, 4, out_l, back_r), (4, 5, out_r, back_l))):
            there, peer = peers[to]
            made.append((there, peers[frm][0], pltpu.make_async_remote_copy(
                src_ref=src.at[g, at], dst_ref=dst.at[g, at], send_sem=back_send.at[k, n],
                recv_sem=back_recv.at[k, n], device_id=peer, device_id_type=MESH,
            )))
        return made

    def lses(g):
        made = []
        for n, (to, frm, src, dst) in enumerate(((5, 4, st_l, lse_r), (4, 5, st_r, lse_l))):
            there, peer = peers[to]
            made.append((there, peers[frm][0], pltpu.make_async_remote_copy(
                src_ref=src.at[g], dst_ref=dst.at[g], send_sem=back_send.at[2 * groups + g, n],
                recv_sem=back_recv.at[2 * groups + g, n], device_id=peer, device_id_type=MESH,
            )))
        return made

    def settings():
        made = []
        plan = ((4, 5, m_right, m_l), (4, 5, d_own, d_l), (5, 4, m_left, m_r), (5, 4, d_own, d_r))
        for n, (to, frm, src, dst) in enumerate(plan):
            there, peer = peers[to]
            made.append((there, peers[frm][0], pltpu.make_async_remote_copy(
                src_ref=src, dst_ref=dst, send_sem=set_send.at[n], recv_sem=set_recv.at[n],
                device_id=peer, device_id_type=MESH,
            )))
        return made

    def each(made, which, act):
        for entry in made:
            @pl.when(entry[which])
            def _():
                act(entry[2])

    each(settings(), 0, lambda copy: copy.start())

    @pl.loop(0, groups)
    def _(g):
        each(copies(g), 0, lambda copy: copy.start())

    for copy in weights:
        copy.start()
    expand_bias(flat_o, m_o, x_o)
    fill_table(0, 0, WINDOW, d_own[0], x_o, t_o)
    each(settings(), 1, lambda copy: copy.wait_recv())
    expand_bias(flat_l, m_l, x_l)
    expand_bias(flat_r, m_r, x_r)
    fill_table(side, RADIUS_MAX + 1, WINDOW, d_l[0], x_l, t_l)
    fill_table(-cols, 0, RADIUS_MAX, d_r[0], x_r, t_r)
    for ref in (l_own, st_l, st_r):
        ref[...] = jnp.zeros_like(ref)
    anchor = row * depth

    @pl.loop(0, 2 * groups)
    def _(k):
        g, part = k // 2, k % 2
        at = pl.ds(pl.multiple_of(g * LANES, LANES), LANES)

        @pl.when(part == 0)
        def _():
            each(copies(g), 1, lambda copy: copy.wait_recv())
            for ref, win, own in ((k_ref, win_k, k_own), (v_ref, win_v, v_own)):
                ref[0:HALO] = win[g, 0:HALO]
                ref[HALO : HALO + depth] = own[:, :, at]
                ref[HALO + depth : 2 * HALO + depth] = win[g, HALO : 2 * HALO]
            q_l[...] = land_l[g]
            q_r[...] = land_r[g]

        @pl.when(k > 0)
        def _():
            each(backs(k - 1), 0, lambda copy: copy.start())

        @pl.when((k > 0) & (part == 0))
        def _():
            each(lses(g - 1), 0, lambda copy: copy.start())

        def put_own(slot, value):
            o_own[slot, :, at] = value

        def put_left(slot, value):
            out_l[g, slot] = value

        def put_right(slot, value):
            out_r[g, slot] = value

        def put_l_own(slot, value):
            l_own[slot] = value

        def put_l_left(slot, value):
            st_l[g] = value

        def put_l_right(slot, value):
            st_r[g] = value

        @pl.loop(0, BLOCKS // 2)
        def _(i):
            beta = part * (BLOCKS // 2) + i
            one_set(d_own[0], anchor, total_rows, g, beta, lambda i: q_ref[i, :, at], t_o, put_own, lambda slot: (l_own[slot], g * GROUP), put_l_own, k_ref, v_ref, s_o, p_o)
            one_set(d_l[0], anchor, total_rows, g, beta, lambda i: q_l[i], t_l, put_left, lambda slot: (st_l[g], slot * GROUP), put_l_left, k_ref, v_ref, s_l, p_l)
            one_set(d_r[0], anchor, total_rows, g, beta, lambda i: q_r[i], t_r, put_right, lambda slot: (st_r[g], slot * GROUP), put_l_right, k_ref, v_ref, s_r, p_r)

    for copy in weights:
        copy.wait()
    each(settings(), 0, lambda copy: copy.wait_send())

    @pl.loop(0, groups)
    def _(g):
        each(copies(g), 0, lambda copy: copy.wait_send())

    each(backs(2 * groups - 1), 0, lambda copy: copy.start())
    each(lses(groups - 1), 0, lambda copy: copy.start())

    @pl.loop(0, groups)
    def _(g):
        each(backs(2 * g), 1, lambda copy: copy.wait_recv())
        each(backs(2 * g + 1), 1, lambda copy: copy.wait_recv())
        each(lses(g), 1, lambda copy: copy.wait_recv())

    def swap(i):
        return pltpu.make_async_remote_copy(
            src_ref=parts.at[i], dst_ref=arrived.at[i], send_sem=head_send.at[i], recv_sem=head_recv.at[i],
            device_id={"head": 1 - head}, device_id_type=MESH,
        )

    steps = parts.shape[0]

    @pl.loop(0, steps)
    def _(i):
        attended[i] = merge_rows(
            i, depth // steps, slots, col > 0, col < cols_n - 1, o_own, back_l, back_r, l_own, lse_l, lse_r
        )

        @pl.when(i > 0)
        def _():
            swap(i - 1).start()

        parts[i] = jnp.dot(attended[i], w_theirs[...], preferred_element_type=jnp.float32).astype(jnp.bfloat16)

    @pl.loop(0, groups)
    def _(g):
        each(backs(2 * g), 0, lambda copy: copy.wait_send())
        each(backs(2 * g + 1), 0, lambda copy: copy.wait_send())
        each(lses(g), 0, lambda copy: copy.wait_send())

    swap(steps - 1).start()

    @pl.loop(0, steps)
    def _(i):
        mine = jnp.dot(attended[i], w_mine[...], preferred_element_type=jnp.float32)
        swap(i).wait_recv()
        result[i] = (mine + arrived[i].astype(jnp.float32)).astype(jnp.bfloat16)

    @pl.loop(0, steps)
    def _(i):
        swap(i).wait_send()


def window_attention(dilation, slots, total_rows, q, k, v, flats, masks, weight):
    depth, cols, features = q.shape
    groups = features // LANES
    heads = groups * GROUP
    keys = BLOCK_KEYS * 32
    half = weight.shape[1] // 2
    steps = 4
    tokens = depth * cols // steps
    counts = (cols, SIDE_COLS, SIDE_COLS)
    vmem = pl.BlockSpec(memory_space=pltpu.VMEM)
    smem = pl.BlockSpec(memory_space=pltpu.SMEM)
    bf16, f32 = jnp.bfloat16, jnp.float32
    dma = pltpu.SemaphoreType.DMA
    return pl.pallas_call(
        functools.partial(window_kernel, total_rows, groups),
        in_specs=[smem, smem] + [vmem] * 9 + [pl.BlockSpec(memory_space=pl.ANY)],
        out_specs=vmem,
        out_shape=jax.ShapeDtypeStruct((steps, tokens, half), bf16),
        scratch_shapes=[
            pltpu.VMEM((SLOTS, cols, features), bf16),
            pltpu.VMEM((SLOTS, cols, 128), f32),
            pltpu.VMEM((groups, SLOTS, SIDE_COLS, LANES), bf16),
            pltpu.VMEM((groups, SLOTS, SIDE_COLS, LANES), bf16),
            pltpu.VMEM((groups, SIDE_COLS, 128), f32),
            pltpu.VMEM((groups, SIDE_COLS, 128), f32),
            pltpu.VMEM((features, half), bf16),
            pltpu.VMEM((features, half), bf16),
            pltpu.VMEM((steps, tokens, features), bf16),
            pltpu.VMEM((steps, tokens, half), bf16),
            pltpu.VMEM((steps, tokens, half), bf16),
        ]
        + [pltpu.VMEM((flat.shape[0] * flat.shape[1], keys), f32) for flat in flats]
        + [pltpu.VMEM((groups, 2 * HALO, cols, LANES), bf16)] * 2
        + [pltpu.VMEM((depth + 2 * HALO, cols, LANES), bf16)] * 2
        + [pltpu.VMEM((groups, depth, SIDE_COLS, LANES), bf16)] * 2
        + [pltpu.VMEM((depth, SIDE_COLS, LANES), bf16)] * 2
        + [pltpu.VMEM((heads, BLOCK_ROWS, n, keys), f32) for n in counts]
        + [pltpu.VMEM((GROUP * BLOCK_ROWS * n, keys), f32) for n in counts]
        + [pltpu.VMEM((GROUP * BLOCK_ROWS * n, keys), bf16) for n in counts]
        + [pltpu.VMEM((groups, SLOTS, SIDE_COLS, LANES), bf16)] * 2
        + [pltpu.VMEM((groups, SIDE_COLS, 128), f32)] * 2
        + [dma((groups, 10)), dma((groups, 10)), dma((3 * groups, 2)), dma((3 * groups, 2))]
        + [dma((steps,)), dma((steps,)), dma((2,))]
        + [pltpu.VMEM(masks[1].shape, f32), pltpu.VMEM(masks[2].shape, f32)]
        + [pltpu.SMEM(dilation.shape, jnp.int32)] * 2
        + [dma((4,)), dma((4,))],
        compiler_params=pltpu.CompilerParams(
            collective_id=0, has_side_effects=True, vmem_limit_bytes=67_000_000
        ),
        cost_estimate=pl.CostEstimate(flops=2 * 10**10, bytes_accessed=4 * 10**7, transcendentals=0),
        name="window_attention",
    )(dilation, slots, q, k, v, *flats, *masks, weight)


def shards(query_map, key_map, value_map, window_mask, tile_radius, dilation_per_tile, rel_bias, out_weight):
    depth, cols, features = query_map.shape
    total_rows = depth * lax.axis_size("row")
    steps = jnp.abs(jnp.arange(WINDOW, dtype=jnp.int32) - RADIUS_MAX)
    centre = (steps[:, None] == 0) & (steps[None, :] == 0)
    radius = tile_radius[0, 0]
    near = (steps[:, None] <= radius) & (steps[None, :] <= radius)
    used = ((window_mask[0, 0] == 1) | centre) & near
    used = jnp.where(used, 0.0, NEG).astype(jnp.float32)[None]
    spans = ((0, WINDOW), (RADIUS_MAX + 1, WINDOW), (0, RADIUS_MAX))
    flats = [block_form(rel_bias, *span, NEG) for span in spans]
    masks = [block_form(used, *span, NEG)[0] for span in spans]
    d = dilation_per_tile[0, 0]
    index = jnp.arange(depth, dtype=jnp.int32)
    turn = index // d
    slots = (d * (turn // BLOCK_ROWS) + index % d) * BLOCK_ROWS + turn % BLOCK_ROWS
    out = window_attention(
        jnp.full((16,), d, jnp.int32), slots.astype(jnp.int32), total_rows,
        query_map, key_map, value_map, flats, masks, out_weight,
    )
    return out.reshape(depth, cols, out.shape[2])


def solution(mesh):
    placed = (
        P("row", "col", "head"),
        P("row", "col", "head"),
        P("row", "col", "head"),
        P("row", "col", None, None),
        P("row", "col"),
        P("row", "col"),
        P("head", None, None),
        P("head", None),
    )
    return jax.shard_map(
        shards, mesh=mesh, in_specs=placed, out_specs=P("row", "col", "head"), check_vma=False
    )
```

```python
import functools

import jax
import jax.numpy as jnp
from jax import lax
from jax.experimental import pallas as pl
from jax.experimental.pallas import tpu as pltpu
from jax.sharding import PartitionSpec as P

HEAD_DIM = 64
RADIUS_MAX = 6
WINDOW = 13
HALO = 18
NEG = -1e30
BLOCK_ROWS = 3
BLOCK_KEYS = 16
SIDE_COLS = 24
GROUP = 4
LANES = GROUP * HEAD_DIM
BLOCKS = 6
SLOTS = BLOCKS * BLOCK_ROWS


MESH = pl.DeviceIdType.MESH


def shifted(value, axis, steps):
    count = lax.axis_size(axis)
    leading, last = (max(0, -steps), min(count, count - steps))
    return lax.ppermute(value, axis, [(source, source + steps) for source in range(leading, last)])


def block_form(value, fill):
    turned = jnp.swapaxes(value, 1, 2)
    extra = BLOCK_KEYS - WINDOW
    count = BLOCK_ROWS * WINDOW
    parts = [
        jnp.pad(turned, ((0, 0), (0, 0), (t, extra - t)), constant_values=fill) for t in range(BLOCK_ROWS)
    ]
    flat = jnp.concatenate(parts, axis=1)
    return jnp.pad(flat, ((0, 0), (0, -count % 8), (0, 0)), constant_values=fill)


def expand_bias(value, x_ref):
    high = value.astype(jnp.bfloat16)
    rest = value - high.astype(jnp.float32)
    middle = rest.astype(jnp.bfloat16)
    low = (rest - middle.astype(jnp.float32)).astype(jnp.bfloat16)
    width = x_ref.shape[1]
    pick = lax.broadcasted_iota(jnp.int32, (BLOCK_KEYS, width), 1) // 32
    pick = (pick == lax.broadcasted_iota(jnp.int32, (BLOCK_KEYS, width), 0)).astype(jnp.bfloat16)
    dot = lambda part: jnp.dot(part, pick, preferred_element_type=jnp.float32)
    x_ref[...] = dot(high) + dot(middle) + dot(low)


def fill_table(offset, first, last, d, x_ref, mask_ref, t_ref):
    heads, _, cols, width = t_ref.shape
    stride = x_ref.shape[0] // heads
    count = last - first

    @pl.loop(0, heads)
    def _(h):
        rows = x_ref[pl.ds(pl.multiple_of(h * stride, 8), stride)] + mask_ref[...]
        for top in range(0, cols, 8):
            lane = lax.broadcasted_iota(jnp.int32, (8, 128), 1)
            rel = lane % 32 - lax.broadcasted_iota(jnp.int32, (8, 128), 0) + (offset - top)
            masks = [rel == (b + first - RADIUS_MAX) * d for b in range(count)]
            for t in range(BLOCK_ROWS):
                for left in range(0, width, 128):
                    acc = jnp.full((8, 128), NEG, jnp.float32)
                    for b in range(count):
                        at = t * WINDOW + first + b
                        acc = jnp.where(masks[b], rows[at : at + 1, left : left + 128], acc)
                    t_ref[h, t, top : top + 8, left : left + 128] = acc


def base_row(beta, d):
    two = beta % 2 + 6 * (beta // 2)
    three = beta % 3 + 9 * (beta // 3)
    return jnp.where(d == 1, 3 * beta, jnp.where(d == 2, two, three))


def one_set(d, row_anchor, total_rows, group, beta, load_q, t_ref, store_o, load_l, store_l, k_ref, v_ref, s_ref, p_ref):
    cols = t_ref.shape[2]
    base = base_row(beta, d)
    span = k_ref.shape[0]
    depth = span - 2 * HALO
    width = BLOCK_KEYS * 32
    queries = []
    for t in range(BLOCK_ROWS):
        row = jnp.minimum(base + t * d, depth - 1)
        queries.append(load_q(row).astype(jnp.float32) * 0.125)
    queries = jnp.concatenate(queries, axis=0)
    lane_head = lax.broadcasted_iota(jnp.int32, queries.shape, 1) // HEAD_DIM
    spread = [jnp.where(lane_head == h, queries, 0.0) for h in range(GROUP)]
    spread = jnp.concatenate(spread, axis=0).astype(jnp.bfloat16)
    key_rows = []
    value_rows = []
    for u in range(BLOCK_KEYS):
        row = jnp.clip(HALO + base + (u - RADIUS_MAX) * d, 0, span - 1)
        key_rows.append(k_ref[row])
        value_rows.append(v_ref[row])
    keys = jnp.concatenate(key_rows, axis=0)
    values = jnp.concatenate(value_rows, axis=0)
    s_ref[...] = lax.dot_general(
        spread, keys, (((1,), (1,)), ((), ())), preferred_element_type=jnp.float32
    )
    step = lax.broadcasted_iota(jnp.int32, (1, width), 1) // 32
    key_row = row_anchor + base + (step - RADIUS_MAX) * d
    row_bias = jnp.where((key_row >= 0) & (key_row < total_rows), 0.0, NEG)
    sums = []
    peaks = []
    for h in range(GROUP):
        for t in range(BLOCK_ROWS):
            at = (h * BLOCK_ROWS + t) * cols
            score = s_ref[at : at + cols] + (t_ref[group * GROUP + h, t] + row_bias)
            peak = jnp.maximum(jnp.max(score, axis=1, keepdims=True), -1e20)
            weight = jnp.exp(score - peak)
            sums.append(jnp.sum(weight, axis=1, keepdims=True))
            peaks.append(peak)
            p_ref[at : at + cols] = weight.astype(jnp.bfloat16)
    mixed = jnp.dot(p_ref[...], values, preferred_element_type=jnp.float32)
    head_of = lax.broadcasted_iota(jnp.int32, (cols, LANES), 1) // HEAD_DIM
    stat_lane = lax.broadcasted_iota(jnp.int32, (cols, 128), 1)
    for t in range(BLOCK_ROWS):
        slot = beta * BLOCK_ROWS + t
        out = jnp.zeros((cols, LANES), jnp.float32)
        stats, lane0 = load_l(slot)
        for h in range(GROUP):
            at = h * BLOCK_ROWS + t
            total = sums[at]
            some = total > 0.0
            inverse = 1.0 / jnp.where(some, total, 1.0)
            out = jnp.where(head_of == h, mixed[at * cols : (at + 1) * cols] * inverse, out)
            lse = jnp.where(some, peaks[at] + jnp.log(jnp.where(some, total, 1.0)), NEG)
            stats = jnp.where(stat_lane == lane0 + h, lse, stats)
        store_o(slot, out.astype(jnp.bfloat16))
        store_l(slot, stats)


def merge_rows(step, rows, slots, has_left, has_right, own, left, right, l_o, l_l, l_r):
    cols, features = own.shape[1:]
    groups = left.shape[0]
    pick = lax.broadcasted_iota(jnp.int32, (128, features), 1) // HEAD_DIM
    pick = (pick == lax.broadcasted_iota(jnp.int32, (128, features), 0)).astype(jnp.bfloat16)
    tail = cols - l_l.shape[1]

    def found(ref, slot):
        lane = lax.broadcasted_iota(jnp.int32, (cols - tail, 128), 1)
        value = jnp.full((cols - tail, 128), NEG, jnp.float32)
        for g in range(groups):
            packed = ref[g]
            for h in range(GROUP):
                one = jnp.sum(jnp.where(lane == slot * GROUP + h, packed, 0.0), axis=1, keepdims=True)
                value = jnp.where(lane == g * GROUP + h, one, value)
        return value

    def lay(value, ahead, fill):
        blank = jnp.full((tail, value.shape[1]), fill, jnp.float32)
        return jnp.concatenate([blank, value] if ahead else [value, blank], axis=0)

    def whole(ref, slot, there):
        value = jnp.concatenate([ref[g, slot].astype(jnp.float32) for g in range(groups)], axis=1)
        return jnp.where(there, value, 0.0)

    first, second, third = [], [], []
    mine, lefts, rights = [], [], []
    for i in range(rows):
        slot = slots[step * rows + i]
        a = l_o[slot]
        b = jnp.where(has_left, lay(found(l_l, slot), False, NEG), NEG)
        c = jnp.where(has_right, lay(found(l_r, slot), True, NEG), NEG)
        top = jnp.maximum(jnp.maximum(a, b), c)
        a, b, c = jnp.exp(a - top), jnp.exp(b - top), jnp.exp(c - top)
        total = a + b + c
        first.append(a / total)
        second.append(b / total)
        third.append(c / total)
        mine.append(own[slot].astype(jnp.float32))
        lefts.append(lay(whole(left, slot, has_left), False, 0.0))
        rights.append(lay(whole(right, slot, has_right), True, 0.0))

    def wide(parts):
        value = jnp.concatenate(parts, axis=0)
        high = value.astype(jnp.bfloat16)
        low = (value - high.astype(jnp.float32)).astype(jnp.bfloat16)
        dot = lambda x: jnp.dot(x, pick, preferred_element_type=jnp.float32)
        return dot(high) + dot(low)

    total = wide(first) * jnp.concatenate(mine, axis=0)
    total = total + wide(second) * jnp.concatenate(lefts, axis=0)
    total = total + wide(third) * jnp.concatenate(rights, axis=0)
    return total.astype(jnp.bfloat16)


def window_kernel(
    total_rows, groups, d_own, slots, q_ref, k_own, v_own, flat, m_o, w_hbm,
    result,
    o_own, l_own, back_l, back_r, lse_l, lse_r, w_theirs, w_mine, attended, parts, arrived, x_all, xm_o, xm_l, xm_r,
    win_k, win_v, k_ref, v_ref, land_l, land_r, q_l, q_r, t_o, t_l, t_r,
    s_o, s_l, s_r, p_o, p_l, p_r, out_l, out_r, st_l, st_r,
    send, recv, back_send, back_recv, head_send, head_recv, w_sem, m_l, m_r, d_l, d_r, set_send, set_recv,
):
    row, col, head = lax.axis_index("row"), lax.axis_index("col"), lax.axis_index("head")
    rows, cols_n = lax.axis_size("row"), lax.axis_size("col")
    depth, cols, _ = k_own.shape
    spill = HALO - depth
    side = land_l.shape[2]
    half = w_mine.shape[1]
    weights = [
        pltpu.make_async_copy(w_hbm.at[:, pl.ds(pl.multiple_of(which * half, 128), half)], dst, w_sem.at[n])
        for n, (which, dst) in enumerate(((1 - head, w_theirs), (head, w_mine)))
    ]

    for edge, at, n in (
        (row < 2, 0, spill),
        (row < 1, spill, depth),
        (row > rows - 2, HALO, depth),
        (row > rows - 3, HALO + depth, spill),
    ):
        @pl.when(edge)
        def _():
            for ref in (win_k, win_v):
                ref[:, at : at + n] = jnp.zeros((groups, n, cols, LANES), ref.dtype)
    for edge, ref, mask, d_ref in ((col < 1, land_l, m_l, d_l), (col > cols_n - 2, land_r, m_r, d_r)):
        @pl.when(edge)
        def _():
            ref[...] = jnp.zeros_like(ref)
            mask[...] = jnp.full(mask.shape, NEG, jnp.float32)
            for n in range(d_ref.shape[0]):
                d_ref[n] = 1

    peers = (
        (row < rows - 1, {"row": row + 1}),
        (row > 0, {"row": row - 1}),
        (row < rows - 2, {"row": row + 2}),
        (row > 1, {"row": row - 2}),
        (col < cols_n - 1, {"col": col + 1}),
        (col > 0, {"col": col - 1}),
    )
    barrier = pltpu.get_barrier_semaphore()
    pl.semaphore_signal(barrier, inc=1, device_id={"head": 1 - head}, device_id_type=MESH)
    count = 1
    for there, peer in peers:
        count = count + there.astype(jnp.int32)

        @pl.when(there)
        def _():
            pl.semaphore_signal(barrier, inc=1, device_id=peer, device_id_type=MESH)
    pl.semaphore_wait(barrier, count)

    def copies(g):
        at = pl.ds(pl.multiple_of(g * LANES, LANES), LANES)
        plan = []
        for own, win in ((k_own, win_k), (v_own, win_v)):
            plan += [
                (0, 1, own.at[:, :, at], win.at[g, spill:HALO]),
                (1, 0, own.at[:, :, at], win.at[g, HALO : HALO + depth]),
                (2, 3, own.at[depth - spill : depth, :, at], win.at[g, 0:spill]),
                (3, 2, own.at[0:spill, :, at], win.at[g, HALO + depth : 2 * HALO]),
            ]
        plan += [
            (4, 5, q_ref.at[:, cols - side : cols, at], land_l.at[g]),
            (5, 4, q_ref.at[:, 0:side, at], land_r.at[g]),
        ]
        made = []
        for n, (to, frm, src, dst) in enumerate(plan):
            there, peer = peers[to]
            made.append((there, peers[frm][0], pltpu.make_async_remote_copy(
                src_ref=src, dst_ref=dst, send_sem=send.at[g, n], recv_sem=recv.at[g, n],
                device_id=peer, device_id_type=MESH,
            )))
        return made

    per = SLOTS // 2

    def backs(k):
        g, at = k // 2, pl.ds((k % 2) * per, per)
        made = []
        for n, (to, frm, src, dst) in enumerate(((5, 4, out_l, back_r), (4, 5, out_r, back_l))):
            there, peer = peers[to]
            made.append((there, peers[frm][0], pltpu.make_async_remote_copy(
                src_ref=src.at[g, at], dst_ref=dst.at[g, at], send_sem=back_send.at[k, n],
                recv_sem=back_recv.at[k, n], device_id=peer, device_id_type=MESH,
            )))
        return made

    def lses(g):
        made = []
        for n, (to, frm, src, dst) in enumerate(((5, 4, st_l, lse_r), (4, 5, st_r, lse_l))):
            there, peer = peers[to]
            made.append((there, peers[frm][0], pltpu.make_async_remote_copy(
                src_ref=src.at[g], dst_ref=dst.at[g], send_sem=back_send.at[2 * groups + g, n],
                recv_sem=back_recv.at[2 * groups + g, n], device_id=peer, device_id_type=MESH,
            )))
        return made

    def settings():
        made = []
        plan = ((4, 5, m_o, m_l), (4, 5, d_own, d_l), (5, 4, m_o, m_r), (5, 4, d_own, d_r))
        for n, (to, frm, src, dst) in enumerate(plan):
            there, peer = peers[to]
            made.append((there, peers[frm][0], pltpu.make_async_remote_copy(
                src_ref=src, dst_ref=dst, send_sem=set_send.at[n], recv_sem=set_recv.at[n],
                device_id=peer, device_id_type=MESH,
            )))
        return made

    def each(made, which, act):
        for entry in made:
            @pl.when(entry[which])
            def _():
                act(entry[2])

    each(settings(), 0, lambda copy: copy.start())

    @pl.loop(0, groups)
    def _(g):
        each(copies(g), 0, lambda copy: copy.start())

    for copy in weights:
        copy.start()
    expand_bias(flat[...].reshape(x_all.shape[0], BLOCK_KEYS), x_all)
    expand_bias(m_o[...], xm_o)
    fill_table(0, 0, WINDOW, d_own[0], x_all, xm_o, t_o)
    each(settings(), 1, lambda copy: copy.wait_recv())
    expand_bias(m_l[...], xm_l)
    expand_bias(m_r[...], xm_r)
    fill_table(side, RADIUS_MAX + 1, WINDOW, d_l[0], x_all, xm_l, t_l)
    fill_table(-cols, 0, RADIUS_MAX, d_r[0], x_all, xm_r, t_r)
    for ref in (l_own, st_l, st_r):
        ref[...] = jnp.zeros_like(ref)
    anchor = row * depth

    @pl.loop(0, 2 * groups)
    def _(k):
        g, part = k // 2, k % 2
        at = pl.ds(pl.multiple_of(g * LANES, LANES), LANES)

        @pl.when(part == 0)
        def _():
            each(copies(g), 1, lambda copy: copy.wait_recv())
            for ref, win, own in ((k_ref, win_k, k_own), (v_ref, win_v, v_own)):
                ref[0:HALO] = win[g, 0:HALO]
                ref[HALO : HALO + depth] = own[:, :, at]
                ref[HALO + depth : 2 * HALO + depth] = win[g, HALO : 2 * HALO]
            q_l[...] = land_l[g]
            q_r[...] = land_r[g]

        @pl.when(k > 0)
        def _():
            each(backs(k - 1), 0, lambda copy: copy.start())

        @pl.when((k > 0) & (part == 0))
        def _():
            each(lses(g - 1), 0, lambda copy: copy.start())

        def put_own(slot, value):
            o_own[slot, :, at] = value

        def put_left(slot, value):
            out_l[g, slot] = value

        def put_right(slot, value):
            out_r[g, slot] = value

        def put_l_own(slot, value):
            l_own[slot] = value

        def put_l_left(slot, value):
            st_l[g] = value

        def put_l_right(slot, value):
            st_r[g] = value

        @pl.loop(0, BLOCKS // 2)
        def _(i):
            beta = part * (BLOCKS // 2) + i
            one_set(d_own[0], anchor, total_rows, g, beta, lambda i: q_ref[i, :, at], t_o, put_own, lambda slot: (l_own[slot], g * GROUP), put_l_own, k_ref, v_ref, s_o, p_o)
            one_set(d_l[0], anchor, total_rows, g, beta, lambda i: q_l[i], t_l, put_left, lambda slot: (st_l[g], slot * GROUP), put_l_left, k_ref, v_ref, s_l, p_l)
            one_set(d_r[0], anchor, total_rows, g, beta, lambda i: q_r[i], t_r, put_right, lambda slot: (st_r[g], slot * GROUP), put_l_right, k_ref, v_ref, s_r, p_r)

    for copy in weights:
        copy.wait()
    each(settings(), 0, lambda copy: copy.wait_send())

    @pl.loop(0, groups)
    def _(g):
        each(copies(g), 0, lambda copy: copy.wait_send())

    each(backs(2 * groups - 1), 0, lambda copy: copy.start())
    each(lses(groups - 1), 0, lambda copy: copy.start())

    @pl.loop(0, groups)
    def _(g):
        each(backs(2 * g), 1, lambda copy: copy.wait_recv())
        each(backs(2 * g + 1), 1, lambda copy: copy.wait_recv())
        each(lses(g), 1, lambda copy: copy.wait_recv())

    def swap(i):
        return pltpu.make_async_remote_copy(
            src_ref=parts.at[i], dst_ref=arrived.at[i], send_sem=head_send.at[i], recv_sem=head_recv.at[i],
            device_id={"head": 1 - head}, device_id_type=MESH,
        )

    steps = parts.shape[0]

    @pl.loop(0, steps)
    def _(i):
        attended[i] = merge_rows(
            i, depth // steps, slots, col > 0, col < cols_n - 1, o_own, back_l, back_r, l_own, lse_l, lse_r
        )

        @pl.when(i > 0)
        def _():
            swap(i - 1).start()

        parts[i] = jnp.dot(attended[i], w_theirs[...], preferred_element_type=jnp.float32).astype(jnp.bfloat16)

    @pl.loop(0, groups)
    def _(g):
        each(backs(2 * g), 0, lambda copy: copy.wait_send())
        each(backs(2 * g + 1), 0, lambda copy: copy.wait_send())
        each(lses(g), 0, lambda copy: copy.wait_send())

    swap(steps - 1).start()

    @pl.loop(0, steps)
    def _(i):
        mine = jnp.dot(attended[i], w_mine[...], preferred_element_type=jnp.float32)
        swap(i).wait_recv()
        result[i] = (mine + arrived[i].astype(jnp.float32)).astype(jnp.bfloat16)

    @pl.loop(0, steps)
    def _(i):
        swap(i).wait_send()


def window_attention(dilation, slots, total_rows, q, k, v, flat, mask, weight):
    depth, cols, features = q.shape
    groups = features // LANES
    heads = groups * GROUP
    keys = BLOCK_KEYS * 32
    half = weight.shape[1] // 2
    steps = 4
    tokens = depth * cols // steps
    counts = (cols, SIDE_COLS, SIDE_COLS)
    vmem = pl.BlockSpec(memory_space=pltpu.VMEM)
    smem = pl.BlockSpec(memory_space=pltpu.SMEM)
    bf16, f32 = jnp.bfloat16, jnp.float32
    dma = pltpu.SemaphoreType.DMA
    return pl.pallas_call(
        functools.partial(window_kernel, total_rows, groups),
        in_specs=[smem, smem] + [vmem] * 5 + [pl.BlockSpec(memory_space=pl.ANY)],
        out_specs=vmem,
        out_shape=jax.ShapeDtypeStruct((steps, tokens, half), bf16),
        scratch_shapes=[
            pltpu.VMEM((SLOTS, cols, features), bf16),
            pltpu.VMEM((SLOTS, cols, 128), f32),
            pltpu.VMEM((groups, SLOTS, SIDE_COLS, LANES), bf16),
            pltpu.VMEM((groups, SLOTS, SIDE_COLS, LANES), bf16),
            pltpu.VMEM((groups, SIDE_COLS, 128), f32),
            pltpu.VMEM((groups, SIDE_COLS, 128), f32),
            pltpu.VMEM((features, half), bf16),
            pltpu.VMEM((features, half), bf16),
            pltpu.VMEM((steps, tokens, features), bf16),
            pltpu.VMEM((steps, tokens, half), bf16),
            pltpu.VMEM((steps, tokens, half), bf16),
        ]
        + [pltpu.VMEM((flat.shape[0] * flat.shape[1], keys), f32)]
        + [pltpu.VMEM((flat.shape[1], keys), f32)] * 3
        + [pltpu.VMEM((groups, 2 * HALO, cols, LANES), bf16)] * 2
        + [pltpu.VMEM((depth + 2 * HALO, cols, LANES), bf16)] * 2
        + [pltpu.VMEM((groups, depth, SIDE_COLS, LANES), bf16)] * 2
        + [pltpu.VMEM((depth, SIDE_COLS, LANES), bf16)] * 2
        + [pltpu.VMEM((heads, BLOCK_ROWS, n, keys), f32) for n in counts]
        + [pltpu.VMEM((GROUP * BLOCK_ROWS * n, keys), f32) for n in counts]
        + [pltpu.VMEM((GROUP * BLOCK_ROWS * n, keys), bf16) for n in counts]
        + [pltpu.VMEM((groups, SLOTS, SIDE_COLS, LANES), bf16)] * 2
        + [pltpu.VMEM((groups, SIDE_COLS, 128), f32)] * 2
        + [dma((groups, 10)), dma((groups, 10)), dma((3 * groups, 2)), dma((3 * groups, 2))]
        + [dma((steps,)), dma((steps,)), dma((2,))]
        + [pltpu.VMEM(mask.shape, f32)] * 2
        + [pltpu.SMEM(dilation.shape, jnp.int32)] * 2
        + [dma((4,)), dma((4,))],
        compiler_params=pltpu.CompilerParams(
            collective_id=0, has_side_effects=True, vmem_limit_bytes=67_000_000
        ),
        cost_estimate=pl.CostEstimate(flops=2 * 10**10, bytes_accessed=4 * 10**7, transcendentals=0),
        name="window_attention",
    )(dilation, slots, q, k, v, flat, mask, weight)


def shards(query_map, key_map, value_map, window_mask, tile_radius, dilation_per_tile, rel_bias, out_weight):
    depth, cols, features = query_map.shape
    total_rows = depth * lax.axis_size("row")
    steps = jnp.abs(jnp.arange(WINDOW, dtype=jnp.int32) - RADIUS_MAX)
    centre = (steps[:, None] == 0) & (steps[None, :] == 0)
    radius = tile_radius[0, 0]
    near = (steps[:, None] <= radius) & (steps[None, :] <= radius)
    used = ((window_mask[0, 0] == 1) | centre) & near
    used = jnp.where(used, 0.0, NEG).astype(jnp.float32)[None]
    flat = block_form(rel_bias, NEG)
    mask = block_form(used, NEG)[0]
    d = dilation_per_tile[0, 0]
    index = jnp.arange(depth, dtype=jnp.int32)
    turn = index // d
    slots = (d * (turn // BLOCK_ROWS) + index % d) * BLOCK_ROWS + turn % BLOCK_ROWS
    out = window_attention(
        jnp.full((16,), d, jnp.int32), slots.astype(jnp.int32), total_rows,
        query_map, key_map, value_map, flat, mask, out_weight,
    )
    return out.reshape(depth, cols, out.shape[2])


def solution(mesh):
    placed = (
        P("row", "col", "head"),
        P("row", "col", "head"),
        P("row", "col", "head"),
        P("row", "col", None, None),
        P("row", "col"),
        P("row", "col"),
        P("head", None, None),
        P("head", None),
    )
    return jax.shard_map(
        shards, mesh=mesh, in_specs=placed, out_specs=P("row", "col", "head"), check_vma=False
    )
```
